256 devices in a mesh: seq: 64 (over z, x, core), head: 4 (over y).
Axes of the slice: x: 4, y: 4, z: 8, core: 2. Of those that a mesh axis runs over, the one named last changes fastest.
Arguments:
- tokens: bfloat16 [65536, 2048], P('seq', 'head'), may hold values from -8 to 8
- w_query: bfloat16 [2048, 2048], P(None, 'head'), may hold values from -1 to 1, as said below
- w_key: bfloat16 [2048, 2048], P(None, 'head'), may hold values from -1 to 1, as said below
- w_value: bfloat16 [2048, 2048], P(None, 'head'), may hold values from -0.125 to 0.125
- w_out: bfloat16 [2048, 2048], P('head'), may hold values from -0.125 to 0.125
- mix_logit: float32 [8], P('head'), may hold values from -2 to 2
Outputs:
- layer_out: bfloat16 [65536, 2048], P('seq', 'head')
The draws below stay inside these ranges and needn't reach their ends.
Inputs may be any that keep to these rules, and one draw needn't show every extreme that they name: `w_query`: entries of mean zero with a standard deviation of about 2048 ** -0.5. `w_key`: entries of mean zero with a standard deviation of about 2048 ** -0.5.
All inputs are finite; a program needn't handle non-finite values.
Results may differ from the reference program's by a relative error of at most 0.0065.
Values may be sent and summed in bfloat16 or wider, within the bound.
A program may use at most 128 MiB of HBM per device.

```python
import jax
import jax.numpy as jnp
from jax import lax

D = 2048
H = 8
DH = 256
SEG_DEV = 1024
TOKENS = 65536


def query_key_pair(key):
    scale = D ** (-0.5)
    base = jnp.clip(jax.random.normal(jax.random.fold_in(key, 31), (D, H * DH), jnp.float32), -4.5, 4.5)
    other = jnp.clip(jax.random.normal(jax.random.fold_in(key, 32), (D, H * DH), jnp.float32), -4.5, 4.5)
    second = other
    return ((base * scale).astype(jnp.bfloat16), (second * scale).astype(jnp.bfloat16))


def draw_w_query(key, part):
    return query_key_pair(key)[0]


def draw_w_key(key, part):
    return query_key_pair(key)[1]


def draw_tokens(key, part):
    nseg = TOKENS // SEG_DEV
    offsets = jax.random.normal(jax.random.fold_in(key, 11), (nseg, 1, D), jnp.float32)
    base = jax.random.normal(jax.random.fold_in(key, 14), (nseg, SEG_DEV, D), jnp.float32)
    whole = base + 0.7 * offsets
    return jnp.clip(whole, -8.0, 8.0).reshape(TOKENS, D).astype(jnp.bfloat16)


def steps_of(stream_key, shape, cuts, smallest, largest):
    loudness, own = 1.0, jax.random.fold_in(stream_key, 6)
    for dim, shards_of in cuts:
        draws = jnp.exp(jax.random.uniform(jax.random.fold_in(own, dim), (shards_of,), jnp.float32, smallest / len(cuts), largest / len(cuts)))
        loudness = loudness * jnp.repeat(draws, shape[dim] // shards_of).reshape([-1 if axis == dim else 1 for axis in range(len(shape))])
    return loudness


def bell_draw(stream_key, shape, scale, limit, split=(), kind=jnp.bfloat16):
    values = scale * jax.random.normal(stream_key, shape, jnp.float32)
    if split:
        values = values * steps_of(stream_key, shape, split, -0.22, 0.18)
    return jnp.clip(values, -limit, limit).astype(kind)


def setup_inputs(seed: int = 0) -> dict:
    key_of = jax.random.split(jax.random.key(seed), 7)
    return {
        "tokens": draw_tokens(jax.random.fold_in(key_of[6], 71), 0),
        "w_query": draw_w_query(jax.random.fold_in(key_of[6], 71), 0),
        "w_key": draw_w_key(jax.random.fold_in(key_of[6], 71), 0),
        "w_value": bell_draw(key_of[3], (D, H * DH), D ** -0.5, 0.125, ((1, 4),)),
        "w_out": bell_draw(key_of[4], (H * DH, D), (H * DH) ** -0.5, 0.125, ((0, 4),)),
        "mix_logit": jnp.clip(jax.random.uniform(key_of[5], (H,), jnp.float32, -2.0, 2.0) * steps_of(key_of[5], (H,), ((0, 4),), -0.4, 0.0), -2.0, 2.0),
    }


def feature(values):
    return jax.nn.elu(values) + 1.0


def reference(tokens, w_query, w_key, w_value, w_out, mix_logit):
    nseg = TOKENS // SEG_DEV
    blocks = tokens.reshape(nseg, SEG_DEV, D)
    share = jax.nn.sigmoid(mix_logit)[None, :, None]
    rows = lax.broadcasted_iota(jnp.int32, (SEG_DEV, SEG_DEV), 0)
    cols = lax.broadcasted_iota(jnp.int32, (SEG_DEV, SEG_DEV), 1)
    causal = cols <= rows
    scale = 1.0 / (DH ** 0.5)

    def one(carry, block):
        memory, normal = carry
        query = jnp.dot(block, w_query, preferred_element_type=jnp.float32).astype(jnp.bfloat16).reshape(SEG_DEV, H, DH)
        keys = jnp.dot(block, w_key, preferred_element_type=jnp.float32).astype(jnp.bfloat16).reshape(SEG_DEV, H, DH)
        values = jnp.dot(block, w_value, preferred_element_type=jnp.float32).astype(jnp.bfloat16).reshape(SEG_DEV, H, DH)
        scores = jnp.einsum("qhd,khd->hqk", query.astype(jnp.float32), keys.astype(jnp.float32)) * scale
        scores = jnp.where(causal[None], scores, -1e30)
        expo = jnp.exp(scores - jnp.max(scores, axis=2, keepdims=True))
        probs = (expo / jnp.sum(expo, axis=2, keepdims=True)).astype(jnp.bfloat16)
        local = jnp.einsum("hqk,khd->qhd", probs.astype(jnp.float32), values.astype(jnp.float32))
        fquery = feature(query.astype(jnp.float32)).astype(jnp.bfloat16).astype(jnp.float32)
        fkey = feature(keys.astype(jnp.float32)).astype(jnp.bfloat16).astype(jnp.float32)
        numer = jnp.einsum("thd,hde->the", fquery, memory, precision=lax.Precision.HIGHEST)
        denom = jnp.einsum("thd,hd->th", fquery, normal, precision=lax.Precision.HIGHEST)
        readout = numer / jnp.maximum(denom, 1.0)[:, :, None]
        mixed = (share * readout + (1.0 - share) * local).astype(jnp.bfloat16).reshape(SEG_DEV, H * DH)
        result = jnp.dot(mixed, w_out, preferred_element_type=jnp.float32).astype(jnp.bfloat16)
        memory = memory + jnp.einsum("thd,the->hde", fkey, values.astype(jnp.float32))
        normal = normal + jnp.sum(fkey, axis=0)
        return (memory, normal), result

    start = (jnp.zeros((H, DH, DH), jnp.float32), jnp.zeros((H, DH), jnp.float32))
    carry, outs = lax.scan(one, start, blocks)
    return outs.reshape(TOKENS, D)
```

```python
import functools

import jax
import jax.numpy as jnp
from jax import lax
from jax.experimental import pallas as pl
from jax.experimental.pallas import tpu as pltpu
from jax.sharding import Mesh
from jax.sharding import PartitionSpec as P

SEQ = ("z", "x", "c")
MESH = pl.DeviceIdType.MESH
F32, BF16 = jnp.float32, jnp.bfloat16
NZ, NX, NC, NY = 8, 4, 2, 4
NE = NX * NC
NU = 2
ZORDER = (1, 7, 2, 6, 3, 5, 4)
NT = (((1,), (1,)), ((), ()))
TN = (((0,), (0,)), ((), ()))


def feature(values):
    return jnp.where(values > 0, values + 1.0, jnp.exp(values))


def kernel(
    tok, wq, wk, wv, wo, logit, out,
    xbuf, wbuf, acc, q_s, k_s, v_s, loc, wof, macc, nacc, mt, ga, tb, gb, pc, gc, mem, mixs, mixr, outs,
    lsem, tsend, trecv, w0s, w0r, w1s, w1r, w2s, w2r, w3s, w3r, asend, arecv, bsend, brecv, csend, crecv,
    msend, mrecv, osend, orecv,
):
    z, x, c, y = (lax.axis_index(a) for a in ("z", "x", "c", "y"))
    e = x * NC + c
    seg, fs = tok.shape
    heads, _, hs = q_s.shape
    rc = seg // 4
    gw = heads * hs
    pr = heads * hs // NE
    br = gw // (NZ * NX)
    half = wo.shape[1] // NC
    rem = lax.rem

    def yy(r):
        return {"y": rem(y + r, NY)}

    def zz(d):
        return {"z": rem(z + d, NZ)}

    def xx(i):
        return {"x": rem(x + i, NX)}

    def ee(i):
        o = rem(e + i, NE)
        return {"x": lax.div(o, NC), "c": rem(o, NC)}

    def remote(src, dst, ssem, rsem, dev):
        return pltpu.make_async_remote_copy(
            src_ref=src, dst_ref=dst, send_sem=ssem, recv_sem=rsem, device_id=dev, device_id_type=MESH
        )

    local = []

    def fetch(src, dst):
        cp = pltpu.make_async_copy(src, dst, lsem.at[len(local)])
        cp.start()
        local.append(cp)

    fetch(tok, xbuf.at[0])
    for r in range(NY):
        rows = pl.ds(pl.multiple_of(rem(y + r, NY) * fs, fs), fs)
        for i, w in enumerate((wk, wv, wq)):
            fetch(w.at[rows, :], wbuf.at[r, :, pl.ds(i * gw, gw)])
    fetch(wo, wof.at[0])

    barrier = pltpu.get_barrier_semaphore()
    peers = [yy(r) for r in range(1, NY)] + [ee(i) for i in range(1, NE)] + [zz(d) for d in range(1, NZ)]
    for dev in peers:
        pl.semaphore_signal(barrier, inc=1, device_id=dev, device_id_type=MESH)
    pl.semaphore_wait(barrier, len(peers))

    def chunk(j):
        return pl.ds(pl.multiple_of(j * rc, rc), rc)

    def t_own(j, way):
        rows = chunk(j if way == 0 else 3 - j)
        return remote(
            tok.at[rows, :], xbuf.at[3 if way == 0 else 1, rows, :],
            tsend.at[way, j], trecv.at[way, j], yy(1 if way == 0 else 3),
        )

    def t_far(j, way):
        rows = chunk(j if way == 0 else 3 - j)
        return remote(
            xbuf.at[3 if way == 0 else 1, rows, :], xbuf.at[2, rows, :],
            tsend.at[way, 4 + j], trecv.at[way, 4 + j], yy(1 if way == 0 else 3),
        )

    cols = pl.ds(pl.multiple_of(c * half, half), half)

    def piece(xp, zp):
        return pl.ds(pl.multiple_of((xp * NZ + zp) * br, br), br)

    def w_y(r):
        return remote(wo.at[piece(x, z), cols], wof.at[NY - r, piece(x, z), cols], w0s.at[r], w0r.at[r], yy(r))

    def w_z(d):
        ref = wof.at[pl.ds(1, NY - 1), piece(x, z), cols]
        return remote(ref, ref, w1s.at[d], w1r.at[d], zz(d))

    def w_x(i, d):
        ref = wof.at[pl.ds(1, NY - 1), piece(x, rem(z + NZ - d, NZ)), cols]
        return remote(ref, ref, w2s.at[i, d], w2r.at[i, d], xx(i))

    def w_c():
        ref = wof.at[pl.ds(1, NY - 1), :, cols]
        return remote(ref, ref, w3s.at[0], w3r.at[0], {"c": 1 - c})

    for r in range(1, NY):
        w_y(r).start()
    for j in range(4):
        t_own(j, 0).start()
        t_own(j, 1).start()

    for cp in local:
        cp.wait()
    macc[...] = jnp.zeros_like(macc)
    nacc[...] = jnp.zeros_like(nacc)
    mt[...] = jnp.zeros_like(mt)

    def own_dot(j, carry):
        rows = chunk(j)
        acc[rows, :] = jnp.dot(xbuf[0, rows, :], wbuf[0], preferred_element_type=F32)
        return carry

    lax.fori_loop(0, 4, own_dot, 0)

    for r in range(1, NY):
        w_y(r).wait_recv()
    for d in ZORDER:
        w_z(d).start()
    for i in range(1, NX):
        w_x(i, 0).start()

    def w_forward(d):
        w_z(d).wait_recv()
        for i in range(1, NX):
            w_x(i, d).start()

    def ring_dot(j, way):
        rows = chunk(j if way == 0 else 3 - j)
        slot = 3 if way == 0 else 1
        acc[rows, :] += jnp.dot(xbuf[slot, rows, :], wbuf[slot], preferred_element_type=F32)

    forward_at = {0: (1, 7), 1: (2, 6), 2: (3, 5), 3: (4,)}
    for j in range(4):
        for way in range(2):
            t_own(j, way).wait_recv()
            if j < 2:
                t_far(j, way).start()
        for d in forward_at[j]:
            w_forward(d)
        for way in range(2):
            ring_dot(j, way)

    def far_rows(rows):
        kv = acc[rows, 0 : 2 * gw] + jnp.dot(xbuf[2, rows, :], wbuf[2, :, 0 : 2 * gw], preferred_element_type=F32)
        kv = kv.astype(BF16)
        for h in range(heads):
            key = kv[:, h * hs : (h + 1) * hs]
            val = kv[:, gw + h * hs : gw + (h + 1) * hs]
            k_s[h, rows, :] = key
            v_s[h, rows, :] = val
            fk = feature(key.astype(F32)).astype(BF16)
            macc[h] += lax.dot_general(fk, val, TN, preferred_element_type=F32)
            nacc[h] += jnp.sum(fk.astype(F32).reshape(rc // 8, 8, hs), axis=0)

    for j in range(2):
        for way in range(2):
            t_far(j, way).wait_recv()
        for way in range(2):
            far_rows(chunk(j if way == 0 else 3 - j))

    per_head = hs // pr
    for h in range(heads):
        norm = jnp.sum(nacc[h], axis=0, keepdims=True)
        norm_rows = jnp.where(lax.broadcasted_iota(jnp.int32, (16, hs), 0) == h, norm, 0.0)
        for p in range(NE):
            if p // per_head == h:
                mt[p, 0:pr, :] = macc[h, (p % per_head) * pr : (p % per_head + 1) * pr, :].astype(BF16)
            mt[p, pr : pr + 16, :] += norm_rows.astype(BF16)

    def a_copy(i):
        return remote(mt.at[rem(e + i, NE)], ga.at[e], asend.at[i], arecv.at[i], ee(i))

    def b_copy(d):
        return remote(tb, gb.at[z], bsend.at[d], brecv.at[d], zz(d))

    def c_copy(i):
        return remote(pc.at[rem(e + i, NE)], gc.at[e], csend.at[i], crecv.at[i], ee(i))

    for i in range(1, NE):
        a_copy(i).start()
    ga[e] = mt[e]

    def q_rows(j, carry):
        rows = chunk(j)
        q = acc[rows, 2 * gw : 3 * gw] + jnp.dot(
            xbuf[2, rows, :], wbuf[2, :, 2 * gw : 3 * gw], preferred_element_type=F32
        )
        q = q.astype(BF16)
        for h in range(heads):
            q_s[h, rows, :] = q[:, h * hs : (h + 1) * hs]
        return carry

    lax.fori_loop(0, 4, q_rows, 0)

    shares = [jax.nn.sigmoid(jnp.full((1, hs), logit[h], F32)) for h in range(heads)]
    scale = 1.0 / hs**0.5
    lower = lax.broadcasted_iota(jnp.int32, (rc, rc), 1) <= lax.broadcasted_iota(jnp.int32, (rc, rc), 0)

    def attend(h):
        for i in range(4):
            rows = slice(i * rc, (i + 1) * rc)
            q = q_s[h, rows, :]
            diag = lax.dot_general(q, k_s[h, rows, :], NT, preferred_element_type=F32) * scale
            diag = jnp.where(lower, diag, -1e30)
            top = jnp.max(diag, axis=1, keepdims=True)
            if i:
                before = lax.dot_general(q, k_s[h, 0 : i * rc, :], NT, preferred_element_type=F32) * scale
                top = jnp.maximum(top, jnp.max(before, axis=1, keepdims=True))
                pb = jnp.exp(before - top)
            pd = jnp.exp(diag - top)
            total = jnp.sum(pd, axis=1, keepdims=True)
            got = jnp.dot(pd.astype(BF16), v_s[h, rows, :], preferred_element_type=F32)
            if i:
                total += jnp.sum(pb, axis=1, keepdims=True)
                got += jnp.dot(pb.astype(BF16), v_s[h, 0 : i * rc, :], preferred_element_type=F32)
            loc[h, rows, :] = got / total * (1.0 - shares[h])

    attend(0)

    for i in range(1, NE):
        a_copy(i).wait_recv()
    plane = ga[0].astype(F32)
    for p in range(1, NE):
        plane += ga[p].astype(F32)
    tb[...] = plane.astype(BF16)
    for d in range(1, NZ):

        @pl.when(z + d < NZ)
        def _(d=d):
            b_copy(d).start()

    attend(1)

    for d in range(1, NZ):

        @pl.when(z - d >= 0)
        def _(d=d):
            b_copy(d).wait_recv()

    run = lax.fori_loop(0, z, lambda k, s: s + gb[k].astype(F32), jnp.zeros(tb.shape, F32))
    for p in range(NE):
        pc[p] = run.astype(BF16)
        run += ga[p].astype(F32)
    for i in range(1, NE):
        c_copy(i).start()
    gc[e] = pc[e]

    for i in range(1, NX):
        for d in range(NZ):
            w_x(i, d).wait_recv()
    w_c().start()

    for i in range(1, NE):
        c_copy(i).wait_recv()
    for p in range(NE):
        mem[p // per_head, (p % per_head) * pr : (p % per_head + 1) * pr, :] = gc[p, 0:pr, :]

    sub = rc // NU

    def m_copy(r, u):
        rows = pl.ds(u * sub, sub)
        return remote(mixs.at[r, rows, :], mixr.at[NY - r, rows, :], msend.at[r, u], mrecv.at[r, u], yy(r))

    def mix(r):
        base = rem(y + r, NY) * rc
        for u in range(NU):
            rows = pl.ds(pl.multiple_of(base + u * sub, sub), sub)
            for h in range(heads):
                fq = feature(q_s[h, rows, :].astype(F32)).astype(BF16)
                norm = jnp.broadcast_to(gc[0, pr + h : pr + h + 1, :], (hs, hs))
                denom = lax.dot_general(fq, norm, NT, preferred_element_type=F32)
                numer = jnp.dot(fq, mem[h], preferred_element_type=F32)
                val = shares[h] * (numer / jnp.maximum(denom, 1.0)) + loc[h, rows, :]
                dst = mixs if r else mixr
                dst[r, u * sub : (u + 1) * sub, h * hs : (h + 1) * hs] = val.astype(BF16)
            if r:
                m_copy(r, u).start()

    for r in (2, 1, 3, 0):
        mix(r)

    w_c().wait_recv()

    def o_copy(r, u):
        rows = pl.ds(pl.multiple_of(y * rc + u * sub, sub), sub)
        return remote(outs.at[r, pl.ds(u * sub, sub), :], out.at[rows, :], osend.at[r, u], orecv.at[r, u], yy(r))

    keep = []
    for u in range(NU):
        rows = slice(u * sub, (u + 1) * sub)
        for r in range(1, NY):
            m_copy(r, u).wait_recv()
        for r in (2, 1, 3, 0):
            oc = pl.ds(pl.multiple_of(rem(y + r, NY) * fs, fs), fs)
            o = jnp.dot(mixr[0, rows, :], wof[0, :, oc], preferred_element_type=F32)
            for s in range(1, NY):
                o += jnp.dot(mixr[s, rows, :], wof[s, :, oc], preferred_element_type=F32)
            outs[r, rows, :] = o.astype(BF16)
            if r:
                o_copy(r, u).start()
            else:
                orows = pl.ds(pl.multiple_of(y * rc + u * sub, sub), sub)
                cp = pltpu.make_async_copy(outs.at[0, pl.ds(u * sub, sub), :], out.at[orows, :], lsem.at[u])
                cp.start()
                keep.append(cp)

    for cp in keep:
        cp.wait()
    for u in range(NU):
        for r in range(1, NY):
            o_copy(r, u).wait_recv()
    for u in range(NU):
        for r in range(1, NY):
            o_copy(r, u).wait_send()
            m_copy(r, u).wait_send()
    for way in range(2):
        for j in range(4):
            t_own(j, way).wait_send()
        for j in range(2):
            t_far(j, way).wait_send()
    for r in range(1, NY):
        w_y(r).wait_send()
    for d in range(1, NZ):
        w_z(d).wait_send()
    for i in range(1, NX):
        for d in range(NZ):
            w_x(i, d).wait_send()
    w_c().wait_send()
    for i in range(1, NE):
        a_copy(i).wait_send()
        c_copy(i).wait_send()
    for d in range(1, NZ):

        @pl.when(z + d < NZ)
        def _(d=d):
            b_copy(d).wait_send()


def on_device(tokens, w_query, w_key, w_value, w_out, mix_logit):
    seg, fs = tokens.shape
    heads = mix_logit.shape[0]
    gw = w_query.shape[1]
    hs = gw // heads
    pr = heads * hs // NE
    rc = seg // 4
    width = w_out.shape[1]
    hbm = pl.BlockSpec(memory_space=pl.ANY)
    dma = pltpu.SemaphoreType.DMA
    return pl.pallas_call(
        kernel,
        out_shape=jax.ShapeDtypeStruct((seg, fs), BF16),
        in_specs=[hbm] * 5 + [pl.BlockSpec(memory_space=pltpu.SMEM)],
        out_specs=hbm,
        scratch_shapes=[
            pltpu.VMEM((NY, seg, fs), BF16),
            pltpu.VMEM((NY, fs, 3 * gw), BF16),
            pltpu.VMEM((seg, 3 * gw), F32),
            pltpu.VMEM((heads, seg, hs), BF16),
            pltpu.VMEM((heads, seg, hs), BF16),
            pltpu.VMEM((heads, seg, hs), BF16),
            pltpu.VMEM((heads, seg, hs), F32),
            pltpu.VMEM((NY, gw, width), BF16),
            pltpu.VMEM((heads, hs, hs), F32),
            pltpu.VMEM((heads, 8, hs), F32),
            pltpu.VMEM((NE, pr + 16, hs), BF16),
            pltpu.VMEM((NE, pr + 16, hs), BF16),
            pltpu.VMEM((pr + 16, hs), BF16),
            pltpu.VMEM((NZ, pr + 16, hs), BF16),
            pltpu.VMEM((NE, pr + 16, hs), BF16),
            pltpu.VMEM((NE, pr + 16, hs), BF16),
            pltpu.VMEM((heads, hs, hs), BF16),
            pltpu.VMEM((NY, rc, gw), BF16),
            pltpu.VMEM((NY, rc, gw), BF16),
            pltpu.VMEM((NY, rc, fs), BF16),
            dma((14,)),
            dma((2, 6)), dma((2, 6)),
            dma((NY,)), dma((NY,)),
            dma((NZ,)), dma((NZ,)),
            dma((NX, NZ)), dma((NX, NZ)),
            dma((1,)), dma((1,)),
            dma((NE,)), dma((NE,)),
            dma((NZ,)), dma((NZ,)),
            dma((NE,)), dma((NE,)),
            dma((NY, NU)), dma((NY, NU)),
            dma((NY, NU)), dma((NY, NU)),
        ],
        compiler_params=pltpu.CompilerParams(
            collective_id=0, has_side_effects=True, vmem_limit_bytes=60 * 2**20
        ),
    )(tokens, w_query, w_key, w_value, w_out, mix_logit)


def solution(mesh):
    torus = Mesh(mesh.devices.reshape(NZ, NX, NC, NY), ("z", "x", "c", "y"))
    return jax.shard_map(
        on_device,
        mesh=torus,
        in_specs=(P(SEQ, "y"), P(None, "y"), P(None, "y"), P(None, "y"), P("y", None), P("y")),
        out_specs=P(SEQ, "y"),
        check_vma=False,
    )
```

```python
import functools

import jax
import jax.numpy as jnp
from jax import lax
from jax.experimental import pallas as pl
from jax.experimental.pallas import tpu as pltpu
from jax.sharding import Mesh
from jax.sharding import PartitionSpec as P

SEQ = ("z", "x", "c")
MESH = pl.DeviceIdType.MESH
F32, BF16 = jnp.float32, jnp.bfloat16
NZ, NX, NC, NY = 8, 4, 2, 4
NE = NX * NC
NU = 2
ZORDER = (1, 7, 2, 6, 3, 5, 4)
NT = (((1,), (1,)), ((), ()))
TN = (((0,), (0,)), ((), ()))


def feature(values):
    return jnp.where(values > 0, values + 1.0, jnp.exp(values))


def kernel(
    tok, wq, wk, wv, wo, logit, out,
    xbuf, wbuf, acc, q_s, k_s, v_s, loc, wof, macc, nacc, mt, ga, tb, gb, pc, gc, mem, mixs, mixr, outs,
    lsem, tsend, trecv, w0s, w0r, w1s, w1r, w2s, w2r, w3s, w3r, asend, arecv, bsend, brecv, csend, crecv,
    msend, mrecv, osend, orecv,
):
    z, x, c, y = (lax.axis_index(a) for a in ("z", "x", "c", "y"))
    e = x * NC + c
    seg, fs = tok.shape
    heads, _, hs = q_s.shape
    rc = seg // 4
    gw = heads * hs
    pr = heads * hs // NE
    br = gw // (NZ * NX)
    half = wo.shape[1] // NC
    rem = lax.rem

    def yy(r):
        return {"y": rem(y + r, NY)}

    def zz(d):
        return {"z": rem(z + d, NZ)}

    def xx(i):
        return {"x": rem(x + i, NX)}

    def ee(i):
        o = rem(e + i, NE)
        return {"x": lax.div(o, NC), "c": rem(o, NC)}

    def remote(src, dst, ssem, rsem, dev):
        return pltpu.make_async_remote_copy(
            src_ref=src, dst_ref=dst, send_sem=ssem, recv_sem=rsem, device_id=dev, device_id_type=MESH
        )

    def fetch(src, dst, k):
        pltpu.make_async_copy(src, dst, lsem.at[k]).start()

    def done(ref, sem):
        pltpu.make_async_copy(ref, ref, sem).wait()

    fetch(tok, xbuf.at[0], 0)
    for r in range(NY):
        rows = pl.ds(pl.multiple_of(rem(y + r, NY) * fs, fs), fs)
        for i, w in enumerate((wk, wv, wq)):
            fetch(w.at[rows, :], wbuf.at[r, :, pl.ds(i * gw, gw)], 1)
    fetch(wo, wof.at[0], 2)

    barrier = pltpu.get_barrier_semaphore()
    peers = [yy(r) for r in range(1, NY)] + [ee(i) for i in range(1, NE)] + [zz(d) for d in range(1, NZ)]
    for dev in peers:
        pl.semaphore_signal(barrier, inc=1, device_id=dev, device_id_type=MESH)
    pl.semaphore_wait(barrier, len(peers))

    def chunk(j):
        return pl.ds(pl.multiple_of(j * rc, rc), rc)

    def t_own(j, way):
        rows = chunk(j if way == 0 else 3 - j)
        return remote(
            tok.at[rows, :], xbuf.at[3 if way == 0 else 1, rows, :],
            tsend.at[0], trecv.at[way, j], yy(1 if way == 0 else 3),
        )

    def t_far(j, way):
        rows = chunk(j if way == 0 else 3 - j)
        return remote(
            xbuf.at[3 if way == 0 else 1, rows, :], xbuf.at[2, rows, :],
            tsend.at[0], trecv.at[way, 4 + j], yy(1 if way == 0 else 3),
        )

    cols = pl.ds(pl.multiple_of(c * half, half), half)

    def piece(xp, zp):
        return pl.ds(pl.multiple_of((xp * NZ + zp) * br, br), br)

    def w_y(r):
        return remote(wo.at[piece(x, z), cols], wof.at[NY - r, piece(x, z), cols], w0s.at[0], w0r.at[0], yy(r))

    def w_z(d):
        ref = wof.at[pl.ds(1, NY - 1), piece(x, z), cols]
        return remote(ref, ref, w1s.at[0], w1r.at[d], zz(d))

    def w_x(i, d):
        ref = wof.at[pl.ds(1, NY - 1), piece(x, rem(z + NZ - d, NZ)), cols]
        return remote(ref, ref, w2s.at[0], w2r.at[0], xx(i))

    def w_c():
        ref = wof.at[pl.ds(1, NY - 1), :, cols]
        return remote(ref, ref, w3s.at[0], w3r.at[0], {"c": 1 - c})

    for r in range(1, NY):
        w_y(r).start()
    for j in range(4):
        t_own(j, 0).start()
        t_own(j, 1).start()

    done(xbuf.at[0], lsem.at[0])
    done(wbuf, lsem.at[1])
    macc[...] = jnp.zeros_like(macc)
    nacc[...] = jnp.zeros_like(nacc)
    mt[...] = jnp.zeros_like(mt)

    def own_dot(j, carry):
        rows = chunk(j)
        acc[rows, :] = jnp.dot(xbuf[0, rows, :], wbuf[0], preferred_element_type=F32)
        return carry

    lax.fori_loop(0, 4, own_dot, 0)

    done(wof.at[pl.ds(1, NY - 1), pl.ds(0, br), cols], w0r.at[0])
    for d in ZORDER:
        w_z(d).start()
    for i in range(1, NX):
        w_x(i, 0).start()

    def w_forward(d):
        w_z(d).wait_recv()
        for i in range(1, NX):
            w_x(i, d).start()

    def ring_dot(j, way):
        rows = chunk(j if way == 0 else 3 - j)
        slot = 3 if way == 0 else 1
        acc[rows, :] += jnp.dot(xbuf[slot, rows, :], wbuf[slot], preferred_element_type=F32)

    forward_at = {0: (1, 7), 1: (2, 6), 2: (3, 5), 3: (4,)}
    for j in range(4):
        for way in range(2):
            t_own(j, way).wait_recv()
            if j < 2:
                t_far(j, way).start()
        for d in forward_at[j]:
            w_forward(d)
        for way in range(2):
            ring_dot(j, way)

    def far_rows(rows):
        kv = acc[rows, 0 : 2 * gw] + jnp.dot(xbuf[2, rows, :], wbuf[2, :, 0 : 2 * gw], preferred_element_type=F32)
        kv = kv.astype(BF16)
        for h in range(heads):
            key = kv[:, h * hs : (h + 1) * hs]
            val = kv[:, gw + h * hs : gw + (h + 1) * hs]
            k_s[h, rows, :] = key
            v_s[h, rows, :] = val
            fk = feature(key.astype(F32)).astype(BF16)
            macc[h] += lax.dot_general(fk, val, TN, preferred_element_type=F32)
            nacc[h] += jnp.sum(fk.astype(F32).reshape(rc // 8, 8, hs), axis=0)

    for j in range(2):
        for way in range(2):
            t_far(j, way).wait_recv()
        for way in range(2):
            far_rows(chunk(j if way == 0 else 3 - j))

    per_head = hs // pr
    for h in range(heads):
        norm = jnp.sum(nacc[h], axis=0, keepdims=True)
        norm_rows = jnp.where(lax.broadcasted_iota(jnp.int32, (16, hs), 0) == h, norm, 0.0)
        for p in range(NE):
            if p // per_head == h:
                mt[p, 0:pr, :] = macc[h, (p % per_head) * pr : (p % per_head + 1) * pr, :].astype(BF16)
            mt[p, pr : pr + 16, :] += norm_rows.astype(BF16)

    def a_copy(i):
        return remote(mt.at[rem(e + i, NE)], ga.at[e], asend.at[0], arecv.at[0], ee(i))

    def b_copy(d):
        return remote(tb, gb.at[z], bsend.at[d], brecv.at[d], zz(d))

    def c_copy(i):
        return remote(pc.at[rem(e + i, NE)], gc.at[e], csend.at[0], crecv.at[0], ee(i))

    for i in range(1, NE):
        a_copy(i).start()
    ga[e] = mt[e]

    def q_rows(j, carry):
        rows = chunk(j)
        q = acc[rows, 2 * gw : 3 * gw] + jnp.dot(
            xbuf[2, rows, :], wbuf[2, :, 2 * gw : 3 * gw], preferred_element_type=F32
        )
        q = q.astype(BF16)
        for h in range(heads):
            q_s[h, rows, :] = q[:, h * hs : (h + 1) * hs]
        return carry

    lax.fori_loop(0, 4, q_rows, 0)

    shares = [jax.nn.sigmoid(jnp.full((1, hs), logit[h], F32)) for h in range(heads)]
    scale = 1.0 / hs**0.5
    lower = lax.broadcasted_iota(jnp.int32, (rc, rc), 1) <= lax.broadcasted_iota(jnp.int32, (rc, rc), 0)

    def attend(h):
        for i in range(4):
            rows = slice(i * rc, (i + 1) * rc)
            q = q_s[h, rows, :]
            diag = lax.dot_general(q, k_s[h, rows, :], NT, preferred_element_type=F32) * scale
            diag = jnp.where(lower, diag, -1e30)
            top = jnp.max(diag, axis=1, keepdims=True)
            if i:
                before = lax.dot_general(q, k_s[h, 0 : i * rc, :], NT, preferred_element_type=F32) * scale
                top = jnp.maximum(top, jnp.max(before, axis=1, keepdims=True))
                pb = jnp.exp(before - top)
            pd = jnp.exp(diag - top)
            total = jnp.sum(pd, axis=1, keepdims=True)
            got = jnp.dot(pd.astype(BF16), v_s[h, rows, :], preferred_element_type=F32)
            if i:
                total += jnp.sum(pb, axis=1, keepdims=True)
                got += jnp.dot(pb.astype(BF16), v_s[h, 0 : i * rc, :], preferred_element_type=F32)
            loc[h, rows, :] = got / total * (1.0 - shares[h])

    attend(0)

    done(ga.at[pl.ds(0, NE - 1)], arecv.at[0])
    plane = ga[0].astype(F32)
    for p in range(1, NE):
        plane += ga[p].astype(F32)
    tb[...] = plane.astype(BF16)
    for d in range(1, NZ):

        @pl.when(z + d < NZ)
        def _(d=d):
            b_copy(d).start()

    attend(1)

    for d in range(1, NZ):

        @pl.when(z - d >= 0)
        def _(d=d):
            b_copy(d).wait_recv()

    run = lax.fori_loop(0, z, lambda k, s: s + gb[k].astype(F32), jnp.zeros(tb.shape, F32))
    for p in range(NE):
        pc[p] = run.astype(BF16)
        run += ga[p].astype(F32)
    for i in range(1, NE):
        c_copy(i).start()
    gc[e] = pc[e]

    done(wof.at[pl.ds(1, NY - 1), pl.ds(0, (NX - 1) * NZ * br), cols], w2r.at[0])
    w_c().start()

    done(gc.at[pl.ds(0, NE - 1)], crecv.at[0])
    for p in range(NE):
        mem[p // per_head, (p % per_head) * pr : (p % per_head + 1) * pr, :] = gc[p, 0:pr, :]

    sub = rc // NU

    def m_copy(r, u):
        rows = pl.ds(u * sub, sub)
        return remote(mixs.at[r, rows, :], mixr.at[NY - r, rows, :], msend.at[0], mrecv.at[u], yy(r))

    def mix(r):
        base = rem(y + r, NY) * rc
        for u in range(NU):
            rows = pl.ds(pl.multiple_of(base + u * sub, sub), sub)
            for h in range(heads):
                fq = feature(q_s[h, rows, :].astype(F32)).astype(BF16)
                norm = jnp.broadcast_to(gc[0, pr + h : pr + h + 1, :], (hs, hs))
                denom = lax.dot_general(fq, norm, NT, preferred_element_type=F32)
                numer = jnp.dot(fq, mem[h], preferred_element_type=F32)
                val = shares[h] * (numer / jnp.maximum(denom, 1.0)) + loc[h, rows, :]
                dst = mixs if r else mixr
                dst[r, u * sub : (u + 1) * sub, h * hs : (h + 1) * hs] = val.astype(BF16)
            if r:
                m_copy(r, u).start()

    for r in (2, 1, 3, 0):
        mix(r)

    w_c().wait_recv()
    done(wof.at[0], lsem.at[2])

    def o_copy(r, u):
        rows = pl.ds(pl.multiple_of(y * rc + u * sub, sub), sub)
        return remote(outs.at[r, pl.ds(u * sub, sub), :], out.at[rows, :], osend.at[0], orecv.at[0], yy(r))

    for u in range(NU):
        rows = slice(u * sub, (u + 1) * sub)
        done(mixr.at[pl.ds(0, NY - 1), pl.ds(0, sub), :], mrecv.at[u])
        for r in (2, 1, 3, 0):
            oc = pl.ds(pl.multiple_of(rem(y + r, NY) * fs, fs), fs)
            o = jnp.dot(mixr[0, rows, :], wof[0, :, oc], preferred_element_type=F32)
            for s in range(1, NY):
                o += jnp.dot(mixr[s, rows, :], wof[s, :, oc], preferred_element_type=F32)
            outs[r, rows, :] = o.astype(BF16)
            if r:
                o_copy(r, u).start()
            else:
                orows = pl.ds(pl.multiple_of(y * rc + u * sub, sub), sub)
                fetch(outs.at[0, pl.ds(u * sub, sub), :], out.at[orows, :], 3)

    three = pl.ds(0, NY - 1)
    done(outs.at[0], lsem.at[3])
    done(outs.at[three], orecv.at[0])
    done(outs.at[three], osend.at[0])
    done(mixs.at[three], msend.at[0])
    done(xbuf.at[three], tsend.at[0])
    done(wof.at[three, pl.ds(0, br), cols], w0s.at[0])
    done(wof.at[three, pl.ds(0, (NZ - 1) * br), cols], w1s.at[0])
    done(wof.at[three, pl.ds(0, (NX - 1) * NZ * br), cols], w2s.at[0])
    w_c().wait_send()
    done(ga.at[pl.ds(0, NE - 1)], asend.at[0])
    done(gc.at[pl.ds(0, NE - 1)], csend.at[0])
    for d in range(1, NZ):

        @pl.when(z + d < NZ)
        def _(d=d):
            b_copy(d).wait_send()


def on_device(tokens, w_query, w_key, w_value, w_out, mix_logit):
    seg, fs = tokens.shape
    heads = mix_logit.shape[0]
    gw = w_query.shape[1]
    hs = gw // heads
    pr = heads * hs // NE
    rc = seg // 4
    width = w_out.shape[1]
    hbm = pl.BlockSpec(memory_space=pl.ANY)
    dma = pltpu.SemaphoreType.DMA
    return pl.pallas_call(
        kernel,
        out_shape=jax.ShapeDtypeStruct((seg, fs), BF16),
        in_specs=[hbm] * 5 + [pl.BlockSpec(memory_space=pltpu.SMEM)],
        out_specs=hbm,
        scratch_shapes=[
            pltpu.VMEM((NY, seg, fs), BF16),
            pltpu.VMEM((NY, fs, 3 * gw), BF16),
            pltpu.VMEM((seg, 3 * gw), F32),
            pltpu.VMEM((heads, seg, hs), BF16),
            pltpu.VMEM((heads, seg, hs), BF16),
            pltpu.VMEM((heads, seg, hs), BF16),
            pltpu.VMEM((heads, seg, hs), F32),
            pltpu.VMEM((NY, gw, width), BF16),
            pltpu.VMEM((heads, hs, hs), F32),
            pltpu.VMEM((heads, 8, hs), F32),
            pltpu.VMEM((NE, pr + 16, hs), BF16),
            pltpu.VMEM((NE, pr + 16, hs), BF16),
            pltpu.VMEM((pr + 16, hs), BF16),
            pltpu.VMEM((NZ, pr + 16, hs), BF16),
            pltpu.VMEM((NE, pr + 16, hs), BF16),
            pltpu.VMEM((NE, pr + 16, hs), BF16),
            pltpu.VMEM((heads, hs, hs), BF16),
            pltpu.VMEM((NY, rc, gw), BF16),
            pltpu.VMEM((NY, rc, gw), BF16),
            pltpu.VMEM((NY, rc, fs), BF16),
            dma((4,)),
            dma((1,)), dma((2, 6)),
            dma((1,)), dma((1,)),
            dma((1,)), dma((NZ,)),
            dma((1,)), dma((1,)),
            dma((1,)), dma((1,)),
            dma((1,)), dma((1,)),
            dma((NZ,)), dma((NZ,)),
            dma((1,)), dma((1,)),
            dma((1,)), dma((NU,)),
            dma((1,)), dma((1,)),
        ],
        compiler_params=pltpu.CompilerParams(
            collective_id=0, has_side_effects=True, vmem_limit_bytes=52 * 2**20
        ),
    )(tokens, w_query, w_key, w_value, w_out, mix_logit)


def solution(mesh):
    torus = Mesh(mesh.devices.reshape(NZ, NX, NC, NY), ("z", "x", "c", "y"))
    return jax.shard_map(
        on_device,
        mesh=torus,
        in_specs=(P(SEQ, "y"), P(None, "y"), P(None, "y"), P(None, "y"), P("y", None), P("y")),
        out_specs=P(SEQ, "y"),
        check_vma=False,
    )
```

```python
import functools

import jax
import jax.numpy as jnp
from jax import lax
from jax.experimental import pallas as pl
from jax.experimental.pallas import tpu as pltpu
from jax.sharding import Mesh
from jax.sharding import PartitionSpec as P

SEQ = ("z", "x", "c")
MESH = pl.DeviceIdType.MESH
F32, BF16 = jnp.float32, jnp.bfloat16
NZ, NX, NC, NY = 8, 4, 2, 4
NE = NX * NC
NU = 8
ZORDER = (1, 7, 2, 6, 3, 5, 4)
NT = (((1,), (1,)), ((), ()))
TN = (((0,), (0,)), ((), ()))


def feature(values):
    return jnp.where(values > 0, values + 1.0, jnp.exp(values))


def kernel(
    tok, wq, wk, wv, wo, logit, out,
    xbuf, wbuf, acc, q_s, k_s, v_s, loc, wof, macc, nacc, mt, ga, tb, gb, pc, gc, mem, mixs, outs, ls, lb,
    lsem, tsend, trecv, wys, wyr, wzs, wzr, wxs, wxr, wcs, wcr, o0s, o0r, o1s, o1r, o2s, o2r, gsend, grecv,
    asend, arecv, bsend, brecv, csend, crecv, psend, precv, dsend, drecv, fsend, frecv, osend, orecv,
):
    z, x, c, y = (lax.axis_index(a) for a in ("z", "x", "c", "y"))
    rem, div = lax.rem, lax.div
    m = div(y, 2)
    part = y + 1 - 2 * rem(y, 2)
    cross = NY - 1 - y
    g = y + c * (cross - y)
    gp = g + 1 - 2 * rem(g, 2)
    e = x * NC + m
    seg, fs = tok.shape
    heads, _, hs = q_s.shape
    rc = seg // 4
    gw = heads * hs
    pr = heads * hs // NE
    br = gw // (NZ * NX)
    wr = NY * fs // (NZ * NX)
    is_main, is_helper = c == m, c != m
    own, other = c == 0, c == 1
    at_home = c + m == 0

    def yy(r):
        return {"y": rem(y + r, NY)}

    def zz(d):
        return {"z": rem(z + d, NZ)}

    def xx(i):
        return {"x": rem(x + i, NX)}

    def ee(i):
        o = rem(e + i, NE)
        par = rem(o, NC)
        diff = par + m - 2 * par * m
        return {"x": div(o, NC), "y": y + diff * (cross - y), "c": c + diff * (1 - 2 * c)}

    sibling = {"c": 1 - c}

    def remote(src, dst, ssem, rsem, dev):
        return pltpu.make_async_remote_copy(
            src_ref=src, dst_ref=dst, send_sem=ssem, recv_sem=rsem, device_id=dev, device_id_type=MESH
        )

    def fetch(src, dst, k):
        pltpu.make_async_copy(src, dst, lsem.at[k]).start()

    def done(ref, sem):
        pltpu.make_async_copy(ref, ref, sem).wait()

    def chunk(j):
        return pl.ds(pl.multiple_of(j * rc, rc), rc)

    def block(f):
        return pl.ds(pl.multiple_of(f * fs, fs), fs)

    def group(f):
        return pl.ds(pl.multiple_of(f * gw, gw), gw)

    which = lax.broadcasted_iota(jnp.int32, ls.shape, 0)
    rows_of = jnp.zeros(ls.shape, F32)
    for h in range(heads):
        rows_of = jnp.where(which == h, logit[h], rows_of)
    ls[...] = rows_of

    weights = (wk, wv, wq)

    @pl.when(is_main)
    def _():
        fetch(tok, xbuf.at[:, block(y)], 0)

    @pl.when(own)
    def _():
        lb[...] = rows_of
        for i, w in enumerate(weights):
            fetch(w, wbuf.at[:, pl.ds(i * gw, gw)], 1)

    fetch(wo.at[:, group(g)], wof.at[0], 2)

    barrier = pltpu.get_barrier_semaphore()
    peers = [yy(r) for r in range(1, NY)] + [ee(i) for i in range(1, NE)] + [zz(d) for d in range(1, NZ)] + [sibling]
    for dev in peers:
        pl.semaphore_signal(barrier, inc=1, device_id=dev, device_id_type=MESH)
    pl.semaphore_wait(barrier, len(peers))

    def t_pair(k):
        return remote(
            tok.at[chunk(k), :], xbuf.at[chunk(k), block(y)], tsend.at[0], trecv.at[0, k], {"y": part}
        )

    def t_cross(k):
        return remote(
            tok.at[chunk(k), :], xbuf.at[chunk(k), block(y)], tsend.at[0], trecv.at[1, k], {"y": cross}
        )

    def t_on(k):
        ref = xbuf.at[chunk(k), block(cross)]
        return remote(ref, ref, tsend.at[0], trecv.at[2, k], {"y": part})

    def t_sib(k, kind, f):
        ref = xbuf.at[chunk(k), block(f)]
        return remote(ref, ref, tsend.at[0], trecv.at[kind, k], sibling)

    def t_own():
        return remote(tok, xbuf.at[:, block(y)], tsend.at[0], trecv.at[3, 0], sibling)

    def t_wait(k, kind, f):
        t_sib(k, kind, f).wait_recv()

    def w_rows(xp, zp):
        return pl.ds(pl.multiple_of((xp * NZ + zp) * wr, wr), wr)

    far_block = rem(x + 2, NX)

    def w_piece(i):
        return remote(
            weights[i].at[w_rows(x, z), :], wbuf.at[w_rows(x, z), pl.ds(i * gw, gw)], wys.at[0], wyr.at[0], {"y": cross}
        )

    def w_z(d):
        ref = wbuf.at[w_rows(x, z), :]
        return remote(ref, ref, wzs.at[0], wzr.at[d], zz(d))

    def w_x(i, d):
        ref = wbuf.at[w_rows(x, rem(z + NZ - d, NZ)), :]
        return remote(ref, ref, wxs.at[0], wxr.at[0], xx(i))

    def w_cross(i):
        return remote(
            weights[i].at[block(far_block), :], wbuf.at[block(far_block), pl.ds(i * gw, gw)],
            wcs.at[0], wcr.at[i // 2], {"y": cross, "c": 1},
        )

    def o_rows(xp, zp):
        return pl.ds(pl.multiple_of((xp * NZ + zp) * br, br), br)

    others = pl.ds(1, NY - 1)

    def o_y(r):
        yt = rem(y + r, NY)
        gt = yt + c * (NY - 1 - 2 * yt)
        return remote(
            wo.at[o_rows(x, z), group(gt)], wof.at[NY - r, o_rows(x, z), :], o0s.at[0], o0r.at[0], yy(r)
        )

    def o_z(d):
        ref = wof.at[others, o_rows(x, z), :]
        return remote(ref, ref, o1s.at[0], o1r.at[0], zz(d))

    def o_x(i):
        ref = wof.at[others, pl.ds(pl.multiple_of(x * NZ * br, NZ * br), NZ * br), :]
        return remote(ref, ref, o2s.at[0], o2r.at[0], xx(i))

    def g_copy():
        return remote(ls, lb, gsend.at[0], grecv.at[0], {"y": cross})

    @pl.when(other)
    def _():
        for i in range(3):
            w_piece(i).start()

    @pl.when(is_main)
    def _():
        for k in range(4):
            t_pair(k).start()
        t_own().start()

    @pl.when(is_helper)
    def _():
        for k in range(4):
            t_cross(k).start()

    for r in range(1, NY):
        o_y(r).start()

    @pl.when(is_helper)
    def _():
        for i in range(3):
            w_cross(i).start()

    @pl.when(other)
    def _():
        g_copy().start()

    macc[...] = jnp.zeros_like(macc)
    nacc[...] = jnp.zeros_like(nacc)
    mt[...] = jnp.zeros_like(mt)

    @pl.when(is_main)
    def _():
        done(xbuf.at[:, block(y)], lsem.at[0])

    @pl.when(is_helper)
    def _():
        t_own().wait_recv()

    @pl.when(own)
    def _():
        done(wbuf, lsem.at[1])

        def own_dot(j, carry):
            acc[chunk(j), :] = jnp.dot(
                xbuf[chunk(j), block(y)], wbuf[block(y), :], preferred_element_type=F32
            )
            return carry

        lax.fori_loop(0, 4, own_dot, 0)

    @pl.when(other)
    def _():
        done(wbuf.at[pl.ds(0, wr), :], wyr.at[0])
        for d in ZORDER:
            w_z(d).start()
        for i in (1, 3):
            w_x(i, 0).start()

    done(wof.at[others, pl.ds(0, br), :], o0r.at[0])
    for d in ZORDER:
        o_z(d).start()

    forward_at = {0: (1, 7), 1: (2, 6), 2: (3, 5), 3: (4,)}
    for k in range(4):
        t_wait(k, 0, part)
        t_wait(k, 1, cross)

        @pl.when(is_main)
        def _(k=k):
            t_on(k).start()
            t_sib(k, 1, cross).start()
            t_sib(k, 0, part).start()

        @pl.when(other)
        def _(k=k):
            for d in forward_at[k]:
                w_z(d).wait_recv()
                for i in (1, 3):
                    w_x(i, d).start()

        @pl.when(own)
        def _(k=k):
            rows = chunk(k)
            add = jnp.dot(xbuf[rows, block(part)], wbuf[block(part), :], preferred_element_type=F32)
            add += jnp.dot(xbuf[rows, block(cross)], wbuf[block(cross), :], preferred_element_type=F32)
            acc[rows, :] += add

    def finish(rows, kv):
        kv = kv.astype(BF16)
        for h in range(heads):
            key = kv[:, h * hs : (h + 1) * hs]
            val = kv[:, gw + h * hs : gw + (h + 1) * hs]
            k_s[h, rows, :] = key
            v_s[h, rows, :] = val
            fk = feature(key.astype(F32)).astype(BF16)
            macc[h] += lax.dot_general(fk, val, TN, preferred_element_type=F32)
            nacc[h] += jnp.sum(fk.astype(F32).reshape(rc // 8, 8, hs), axis=0)

    last = NY - 1 - part
    for k in range(4):
        t_wait(k, 2, last)

        @pl.when(is_main)
        def _(k=k):
            t_sib(k, 2, last).start()

        if k == 1:
            done(wof.at[others, pl.ds(0, (NZ - 1) * br), :], o1r.at[0])

            @pl.when(own)
            def _():
                for i in range(1, NX):
                    o_x(i).start()

        @pl.when(own)
        def _(k=k):
            rows = chunk(k)
            add = jnp.dot(xbuf[rows, block(last)], wbuf[block(last), 0 : 2 * gw], preferred_element_type=F32)
            finish(rows, acc[rows, 0 : 2 * gw] + add)

    @pl.when(other)
    def _():
        done(wbuf.at[pl.ds(0, 2 * NZ * wr), :], wxr.at[0])
        done(wbuf.at[pl.ds(0, fs), pl.ds(0, 2 * gw)], wcr.at[0])

        def whole(j, carry):
            rows = chunk(j)
            finish(rows, jnp.dot(xbuf[rows, :], wbuf[:, 0 : 2 * gw], preferred_element_type=F32))
            return carry

        lax.fori_loop(0, 4, whole, 0)

    per_head = hs // pr
    for h in range(heads):
        norm = jnp.sum(nacc[h], axis=0, keepdims=True)
        norm_rows = jnp.where(lax.broadcasted_iota(jnp.int32, (16, hs), 0) == h, norm, 0.0)
        for p in range(NE):
            if p // per_head == h:
                mt[p, 0:pr, :] = macc[h, (p % per_head) * pr : (p % per_head + 1) * pr, :].astype(BF16)
            mt[p, pr : pr + 16, :] += norm_rows.astype(BF16)

    def a_copy(i):
        return remote(mt.at[rem(e + i, NE)], ga.at[e], asend.at[0], arecv.at[0], ee(i))

    def b_copy(d):
        return remote(tb, gb.at[z], bsend.at[d], brecv.at[d], zz(d))

    def c_copy(i):
        return remote(pc.at[rem(e + i, NE)], gc.at[e], csend.at[0], crecv.at[0], ee(i))

    for i in range(1, NE):
        a_copy(i).start()
    ga[e] = mt[e]

    def put_q(rows, q):
        q = q.astype(BF16)
        for h in range(heads):
            q_s[h, rows, :] = q[:, h * hs : (h + 1) * hs]

    @pl.when(own)
    def _():
        def q_rows(j, carry):
            rows = chunk(j)
            add = jnp.dot(xbuf[rows, block(last)], wbuf[block(last), 2 * gw : 3 * gw], preferred_element_type=F32)
            put_q(rows, acc[rows, 2 * gw : 3 * gw] + add)
            return carry

        lax.fori_loop(0, 4, q_rows, 0)

    @pl.when(other)
    def _():
        done(wbuf.at[pl.ds(0, fs), pl.ds(2 * gw, gw)], wcr.at[1])
        g_copy().wait_recv()

        def q_rows(j, carry):
            rows = chunk(j)
            put_q(rows, jnp.dot(xbuf[rows, :], wbuf[:, 2 * gw : 3 * gw], preferred_element_type=F32))
            return carry

        lax.fori_loop(0, 4, q_rows, 0)

    shares = [jax.nn.sigmoid(lb[h : h + 1, :]) for h in range(heads)]
    scale = 1.0 / hs**0.5
    lower = lax.broadcasted_iota(jnp.int32, (rc, rc), 1) <= lax.broadcasted_iota(jnp.int32, (rc, rc), 0)

    def attend(h):
        for i in range(4):
            rows = slice(i * rc, (i + 1) * rc)
            q = q_s[h, rows, :]
            diag = lax.dot_general(q, k_s[h, rows, :], NT, preferred_element_type=F32) * scale
            diag = jnp.where(lower, diag, -1e30)
            top = jnp.max(diag, axis=1, keepdims=True)
            if i:
                before = lax.dot_general(q, k_s[h, 0 : i * rc, :], NT, preferred_element_type=F32) * scale
                top = jnp.maximum(top, jnp.max(before, axis=1, keepdims=True))
                pb = jnp.exp(before - top)
            pd = jnp.exp(diag - top)
            total = jnp.sum(pd, axis=1, keepdims=True)
            got = jnp.dot(pd.astype(BF16), v_s[h, rows, :], preferred_element_type=F32)
            if i:
                total += jnp.sum(pb, axis=1, keepdims=True)
                got += jnp.dot(pb.astype(BF16), v_s[h, 0 : i * rc, :], preferred_element_type=F32)
            loc[h, rows, :] = got / total * (1.0 - shares[h])

    attend(0)

    done(ga.at[pl.ds(0, NE - 1)], arecv.at[0])
    plane = ga[0].astype(F32)
    for p in range(1, NE):
        plane += ga[p].astype(F32)
    tb[...] = plane.astype(BF16)
    for d in range(1, NZ):

        @pl.when(z + d < NZ)
        def _(d=d):
            b_copy(d).start()

    attend(1)

    for d in range(1, NZ):

        @pl.when(z - d >= 0)
        def _(d=d):
            b_copy(d).wait_recv()

    run = lax.fori_loop(0, z, lambda k, s: s + gb[k].astype(F32), jnp.zeros(tb.shape, F32))
    for p in range(NE):
        pc[p] = run.astype(BF16)
        run += ga[p].astype(F32)
    for i in range(1, NE):
        c_copy(i).start()
    gc[e] = pc[e]

    @pl.when(other)
    def _():
        for i in range(1, NX):
            o_x(i).start()

    done(gc.at[pl.ds(0, NE - 1)], crecv.at[0])
    for p in range(NE):
        mem[p // per_head, (p % per_head) * pr : (p % per_head + 1) * pr, :] = gc[p, 0:pr, :]

    sub = seg // NU

    def m_ref(u, f):
        return mixs.at[pl.ds(u * sub, sub), group(f)]

    def m_pair(u, f):
        return remote(m_ref(u, f), m_ref(u, f), psend.at[0], precv.at[u], {"y": part})

    def m_sib(u, f):
        return remote(m_ref(u, f), m_ref(u, f), dsend.at[0], drecv.at[u], sibling)

    def m_on(u, f):
        return remote(m_ref(u, f), m_ref(u, f), fsend.at[0], frecv.at[u], sibling)

    for u in range(NU):
        rows = pl.ds(u * sub, sub)
        for h in range(heads):
            fq = feature(q_s[h, rows, :].astype(F32)).astype(BF16)
            norm = jnp.broadcast_to(gc[0, pr + h : pr + h + 1, :], (hs, hs))
            denom = lax.dot_general(fq, norm, NT, preferred_element_type=F32)
            numer = jnp.dot(fq, mem[h], preferred_element_type=F32)
            val = shares[h] * (numer / jnp.maximum(denom, 1.0)) + loc[h, rows, :]
            mixs[rows, pl.ds(pl.multiple_of(g * gw + h * hs, hs), hs)] = val.astype(BF16)
        m_pair(u, g).start()
        m_sib(u, g).start()

    done(wof.at[others, pl.ds(0, (NX - 1) * NZ * br), :], o2r.at[0])
    done(wof.at[0], lsem.at[2])

    def o_copy(u):
        rows = pl.ds(u * sub, sub)
        dev = {"y": y + c * (cross - y), "c": m}
        return remote(outs.at[rows, :], out.at[rows, :], osend.at[0], orecv.at[0], dev)

    for step in range(NU + 1):
        if step < NU:
            m_pair(step, gp).wait_recv()
            m_on(step, gp).start()
        if step:
            u = step - 1
            rows = pl.ds(u * sub, sub)
            m_sib(u, NY - 1 - g).wait_recv()
            m_on(u, NY - 1 - gp).wait_recv()
            o = jnp.dot(mixs[rows, group(y)], wof[0], preferred_element_type=F32)
            for r in range(1, NY):
                o += jnp.dot(mixs[rows, group(rem(y + r, NY))], wof[r], preferred_element_type=F32)
            outs[rows, :] = o.astype(BF16)

            @pl.when(at_home)
            def _(rows=rows):
                fetch(outs.at[rows, :], out.at[rows, :], 3)

            @pl.when(jnp.logical_not(at_home))
            def _(u=u):
                o_copy(u).start()

    @pl.when(at_home)
    def _():
        done(outs, lsem.at[3])

    @pl.when(jnp.logical_not(at_home))
    def _():
        done(outs, osend.at[0])

    @pl.when(jnp.logical_not(at_home))
    def _():
        done(outs, orecv.at[0])

    done(outs, psend.at[0])
    done(outs, dsend.at[0])
    done(outs, fsend.at[0])

    @pl.when(is_main)
    def _():
        done(wbuf, tsend.at[0])

    @pl.when(is_helper)
    def _():
        done(xbuf.at[:, pl.ds(0, fs)], tsend.at[0])
        done(wbuf.at[pl.ds(0, fs), :], wcs.at[0])

    @pl.when(other)
    def _():
        done(wbuf.at[pl.ds(0, wr), :], wys.at[0])
        done(wbuf.at[pl.ds(0, (NZ - 1) * wr), :], wzs.at[0])
        done(wbuf.at[pl.ds(0, 2 * NZ * wr), :], wxs.at[0])
        g_copy().wait_send()

    done(wof.at[others, pl.ds(0, br), :], o0s.at[0])
    done(wof.at[others, pl.ds(0, (NZ - 1) * br), :], o1s.at[0])
    done(wof.at[others, pl.ds(0, (NX - 1) * NZ * br), :], o2s.at[0])
    done(ga.at[pl.ds(0, NE - 1)], asend.at[0])
    done(gc.at[pl.ds(0, NE - 1)], csend.at[0])
    for d in range(1, NZ):

        @pl.when(z + d < NZ)
        def _(d=d):
            b_copy(d).wait_send()


def on_device(tokens, w_query, w_key, w_value, w_out, mix_logit):
    seg, fs = tokens.shape
    heads = mix_logit.shape[0]
    gw = w_query.shape[1]
    hs = gw // heads
    pr = heads * hs // NE
    hbm = pl.BlockSpec(memory_space=pl.ANY)
    dma = pltpu.SemaphoreType.DMA
    return pl.pallas_call(
        kernel,
        out_shape=jax.ShapeDtypeStruct((seg, fs), BF16),
        in_specs=[hbm] * 5 + [pl.BlockSpec(memory_space=pltpu.SMEM)],
        out_specs=hbm,
        scratch_shapes=[
            pltpu.VMEM((seg, NY * fs), BF16),
            pltpu.VMEM((NY * fs, 3 * gw), BF16),
            pltpu.VMEM((seg, 3 * gw), F32),
            pltpu.VMEM((heads, seg, hs), BF16),
            pltpu.VMEM((heads, seg, hs), BF16),
            pltpu.VMEM((heads, seg, hs), BF16),
            pltpu.VMEM((heads, seg, hs), F32),
            pltpu.VMEM((NY, gw, fs), BF16),
            pltpu.VMEM((heads, hs, hs), F32),
            pltpu.VMEM((heads, 8, hs), F32),
            pltpu.VMEM((NE, pr + 16, hs), BF16),
            pltpu.VMEM((NE, pr + 16, hs), BF16),
            pltpu.VMEM((pr + 16, hs), BF16),
            pltpu.VMEM((NZ, pr + 16, hs), BF16),
            pltpu.VMEM((NE, pr + 16, hs), BF16),
            pltpu.VMEM((NE, pr + 16, hs), BF16),
            pltpu.VMEM((heads, hs, hs), BF16),
            pltpu.VMEM((seg, NY * gw), BF16),
            pltpu.VMEM((seg, fs), BF16),
            pltpu.VMEM((8, hs), F32),
            pltpu.VMEM((8, hs), F32),
            dma((4,)),
            dma((1,)), dma((4, 4)),
            dma((1,)), dma((1,)),
            dma((1,)), dma((NZ,)),
            dma((1,)), dma((1,)),
            dma((1,)), dma((2,)),
            dma((1,)), dma((1,)),
            dma((1,)), dma((1,)),
            dma((1,)), dma((1,)),
            dma((1,)), dma((1,)),
            dma((1,)), dma((1,)),
            dma((NZ,)), dma((NZ,)),
            dma((1,)), dma((1,)),
            dma((1,)), dma((NU,)),
            dma((1,)), dma((NU,)),
            dma((1,)), dma((NU,)),
            dma((1,)), dma((1,)),
        ],
        compiler_params=pltpu.CompilerParams(
            collective_id=0, has_side_effects=True, vmem_limit_bytes=52 * 2**20
        ),
    )(tokens, w_query, w_key, w_value, w_out, mix_logit)


def solution(mesh):
    torus = Mesh(mesh.devices.reshape(NZ, NX, NC, NY), ("z", "x", "c", "y"))
    return jax.shard_map(
        on_device,
        mesh=torus,
        in_specs=(P(SEQ, "y"), P(None, "y"), P(None, "y"), P(None, "y"), P("y", None), P("y")),
        out_specs=P(SEQ, "y"),
        check_vma=False,
    )
```

```python
import functools

import jax
import jax.numpy as jnp
from jax import lax
from jax.experimental import pallas as pl
from jax.experimental.pallas import tpu as pltpu
from jax.sharding import Mesh
from jax.sharding import PartitionSpec as P

SEQ = ("z", "x", "c")
MESH = pl.DeviceIdType.MESH
F32, BF16 = jnp.float32, jnp.bfloat16
NZ, NX, NC, NY = 8, 4, 2, 4
NE = NX * NC
NU = 9
ZORDER = (1, 7, 2, 6, 3, 5, 4)
NT = (((1,), (1,)), ((), ()))
TN = (((0,), (0,)), ((), ()))


def feature(values):
    return jnp.where(values > 0, values + 1.0, jnp.exp(values))


def kernel(
    tok, wq, wk, wv, wo, logit, out,
    xbuf, wbuf, acc, q_s, k_s, v_s, loc, wof, macc, nacc, mt, ga, tb, gb, pc, gc, mem, mixs, outs, ls, lb,
    lsem, tsend, trecv, wys, wyr, wzs, wzr, wxs, wxr, wcs, wcr, o0s, o0r, o1s, o1r, o2s, o2r, o3s, o3r, gsend, grecv,
    asend, arecv, bsend, brecv, csend, crecv, psend, precv, dsend, drecv, fsend, frecv, osend, orecv,
):
    z, x, c, y = (lax.axis_index(a) for a in ("z", "x", "c", "y"))
    rem, div = lax.rem, lax.div
    m = div(y, 2)
    part = y + 1 - 2 * rem(y, 2)
    cross = NY - 1 - y
    g = y + c * (cross - y)
    gp = g + 1 - 2 * rem(g, 2)
    e = x * NC + m
    seg, fs = tok.shape
    heads, _, hs = q_s.shape
    rc = seg // 4
    gw = heads * hs
    pr = heads * hs // NE
    br = gw // (NZ * NX)
    wr = NY * fs // (NZ * NX)
    is_main, is_helper = c == m, c != m
    own, other = c == 0, c == 1
    at_home = c + m == 0

    def yy(r):
        return {"y": rem(y + r, NY)}

    def zz(d):
        return {"z": rem(z + d, NZ)}

    def xx(i):
        return {"x": rem(x + i, NX)}

    def ee(i):
        o = rem(e + i, NE)
        par = rem(o, NC)
        diff = par + m - 2 * par * m
        return {"x": div(o, NC), "y": y + diff * (cross - y), "c": c + diff * (1 - 2 * c)}

    sibling = {"c": 1 - c}

    def remote(src, dst, ssem, rsem, dev):
        return pltpu.make_async_remote_copy(
            src_ref=src, dst_ref=dst, send_sem=ssem, recv_sem=rsem, device_id=dev, device_id_type=MESH
        )

    def fetch(src, dst, k):
        pltpu.make_async_copy(src, dst, lsem.at[k]).start()

    def done(ref, sem):
        pltpu.make_async_copy(ref, ref, sem).wait()

    def chunk(j):
        return pl.ds(pl.multiple_of(j * rc, rc), rc)

    def block(f):
        return pl.ds(pl.multiple_of(f * fs, fs), fs)

    def group(f):
        return pl.ds(pl.multiple_of(f * gw, gw), gw)

    barrier = pltpu.get_barrier_semaphore()
    peers = [zz(d) for d in range(1, NZ)] + [yy(r) for r in range(1, NY)] + [ee(i) for i in range(1, NE)] + [sibling]
    for dev in peers:
        pl.semaphore_signal(barrier, inc=1, device_id=dev, device_id_type=MESH)

    which = lax.broadcasted_iota(jnp.int32, ls.shape, 0)
    rows_of = jnp.zeros(ls.shape, F32)
    for h in range(heads):
        rows_of = jnp.where(which == h, logit[h], rows_of)
    ls[...] = rows_of

    weights = (wk, wv, wq)

    @pl.when(is_main)
    def _():
        fetch(tok, xbuf.at[:, block(y)], 0)

    @pl.when(own)
    def _():
        lb[...] = rows_of
        for i, w in enumerate(weights):
            fetch(w, wbuf.at[:, pl.ds(i * gw, gw)], 1)

    fetch(wo.at[:, group(g)], wof.at[0], 2)

    pl.semaphore_wait(barrier, len(peers))

    def t_pair(k):
        return remote(
            tok.at[chunk(k), :], xbuf.at[chunk(k), block(y)], tsend.at[0], trecv.at[0, k], {"y": part}
        )

    def t_cross(k):
        return remote(
            tok.at[chunk(k), :], xbuf.at[chunk(k), block(y)], tsend.at[0], trecv.at[1, k], {"y": cross}
        )

    def t_on(k):
        ref = xbuf.at[chunk(k), block(cross)]
        return remote(ref, ref, tsend.at[0], trecv.at[2, k], {"y": part})

    def t_sib(k, kind, f):
        ref = xbuf.at[chunk(k), block(f)]
        return remote(ref, ref, tsend.at[0], trecv.at[kind, k], sibling)

    def t_own():
        return remote(tok, xbuf.at[:, block(y)], tsend.at[0], trecv.at[3, 0], sibling)

    def t_wait(k, kind, f):
        t_sib(k, kind, f).wait_recv()

    def w_rows(xp, zp):
        return pl.ds(pl.multiple_of((xp * NZ + zp) * wr, wr), wr)

    far_block = rem(x + 2, NX)

    def w_piece(i):
        return remote(
            weights[i].at[w_rows(x, z), :], wbuf.at[w_rows(x, z), pl.ds(i * gw, gw)], wys.at[0], wyr.at[i // 2], {"y": cross}
        )

    w_cols = (pl.ds(0, 2 * gw), pl.ds(2 * gw, gw))

    def w_z(kind, d):
        ref = wbuf.at[w_rows(x, z), w_cols[kind]]
        return remote(ref, ref, wzs.at[0], wzr.at[kind, d], zz(d))

    def w_x(kind, i, d):
        ref = wbuf.at[w_rows(x, rem(z + NZ - d, NZ)), w_cols[kind]]
        return remote(ref, ref, wxs.at[0], wxr.at[kind], xx(i))

    def w_cross(i):
        return remote(
            weights[i].at[block(far_block), :], wbuf.at[block(far_block), pl.ds(i * gw, gw)],
            wcs.at[0], wcr.at[i // 2], {"y": cross, "c": 1},
        )

    def o_rows(xp, zp):
        return pl.ds(pl.multiple_of((xp * NZ + zp) * br, br), br)

    def o_y():
        return remote(
            wo.at[o_rows(x, z), group(NY - 1 - gp)], wof.at[2, o_rows(x, z), :], o0s.at[0], o0r.at[0], yy(2)
        )

    def o_z(d):
        ref = wof.at[2, o_rows(x, z), :]
        return remote(ref, ref, o1s.at[0], o1r.at[0], zz(d))

    def o_x(i):
        ref = wof.at[2, pl.ds(pl.multiple_of(x * NZ * br, NZ * br), NZ * br), :]
        return remote(ref, ref, o2s.at[0], o2r.at[0], xx(i))

    def o_pair():
        return remote(
            wo.at[:, group(gp)], wof.at[3 - 2 * rem(y, 2)], o3s.at[0], o3r.at[0], {"y": part}
        )

    def o_cross():
        return remote(
            wo.at[:, group(NY - 1 - g)], wof.at[1 + 2 * rem(y, 2)], o3s.at[0], o3r.at[1], {"y": cross}
        )

    def g_copy():
        return remote(ls, lb, gsend.at[0], grecv.at[0], {"y": cross})

    @pl.when(other)
    def _():
        for i in range(3):
            w_piece(i).start()

    o_y().start()

    @pl.when(is_main)
    def _():
        for k in range(4):
            t_pair(k).start()
        t_own().start()

    @pl.when(is_helper)
    def _():
        for k in range(4):
            t_cross(k).start()
        for i in range(3):
            w_cross(i).start()

    @pl.when(other)
    def _():
        g_copy().start()

    macc[...] = jnp.zeros_like(macc)
    nacc[...] = jnp.zeros_like(nacc)
    mt[...] = jnp.zeros_like(mt)

    @pl.when(is_main)
    def _():
        done(xbuf.at[:, block(y)], lsem.at[0])

    @pl.when(is_helper)
    def _():
        t_own().wait_recv()

    @pl.when(own)
    def _():
        done(wbuf, lsem.at[1])

        def own_dot(j, carry):
            acc[chunk(j), :] = jnp.dot(
                xbuf[chunk(j), block(y)], wbuf[block(y), :], preferred_element_type=F32
            )
            return carry

        lax.fori_loop(0, 4, own_dot, 0)

    @pl.when(other)
    def _():
        done(wbuf.at[pl.ds(0, wr), pl.ds(0, 2 * gw)], wyr.at[0])
        for d in ZORDER:
            w_z(0, d).start()
        for i in (1, 3):
            w_x(0, i, 0).start()

    forward_at = {0: (1, 7), 1: (2, 6), 2: (3, 5), 3: (4,)}
    for k in range(4):
        t_wait(k, 0, part)
        t_wait(k, 1, cross)

        @pl.when(is_main)
        def _(k=k):
            t_on(k).start()
            t_sib(k, 1, cross).start()
            t_sib(k, 0, part).start()

        @pl.when(other)
        def _(k=k):
            for d in forward_at[k]:
                w_z(0, d).wait_recv()
                for i in (1, 3):
                    w_x(0, i, d).start()

        @pl.when(own)
        def _(k=k):
            rows = chunk(k)
            add = jnp.dot(xbuf[rows, block(part)], wbuf[block(part), :], preferred_element_type=F32)
            add += jnp.dot(xbuf[rows, block(cross)], wbuf[block(cross), :], preferred_element_type=F32)
            acc[rows, :] += add

    def finish(rows, kv):
        kv = kv.astype(BF16)
        for h in range(heads):
            key = kv[:, h * hs : (h + 1) * hs]
            val = kv[:, gw + h * hs : gw + (h + 1) * hs]
            k_s[h, rows, :] = key
            v_s[h, rows, :] = val
            fk = feature(key.astype(F32)).astype(BF16)
            macc[h] += lax.dot_general(fk, val, TN, preferred_element_type=F32)
            nacc[h] += jnp.sum(fk.astype(F32).reshape(rc // 8, 8, hs), axis=0)

    @pl.when(other)
    def _():
        done(wbuf.at[pl.ds(0, wr), pl.ds(0, gw)], wyr.at[1])
        for d in ZORDER:
            w_z(1, d).start()
        for i in (1, 3):
            w_x(1, i, 0).start()

    done(wof.at[2, pl.ds(0, br), :], o0r.at[0])
    for d in ZORDER:
        o_z(d).start()

    last = NY - 1 - part
    for k in range(4):
        t_wait(k, 2, last)

        @pl.when(is_main)
        def _(k=k):
            t_sib(k, 2, last).start()

        @pl.when(other)
        def _(k=k):
            rows = chunk(k)
            acc[rows, 0 : 2 * gw] = jnp.dot(
                xbuf[rows, block(x)], wbuf[block(x), 0 : 2 * gw], preferred_element_type=F32
            )

        @pl.when(own)
        def _(k=k):
            rows = chunk(k)
            add = jnp.dot(xbuf[rows, block(last)], wbuf[block(last), 0 : 2 * gw], preferred_element_type=F32)
            finish(rows, acc[rows, 0 : 2 * gw] + add)

    @pl.when(other)
    def _():
        for d in ZORDER:
            w_z(1, d).wait_recv()
            for i in (1, 3):
                w_x(1, i, d).start()
        done(wbuf.at[pl.ds(0, 2 * NZ * wr), pl.ds(0, 2 * gw)], wxr.at[0])
        done(wbuf.at[pl.ds(0, fs), pl.ds(0, 2 * gw)], wcr.at[0])

        def whole(j, carry):
            rows = chunk(j)
            kv = acc[rows, 0 : 2 * gw]
            for i in range(1, NX):
                f = block(rem(x + i, NX))
                kv += jnp.dot(xbuf[rows, f], wbuf[f, 0 : 2 * gw], preferred_element_type=F32)
            finish(rows, kv)
            return carry

        lax.fori_loop(0, 4, whole, 0)

    per_head = hs // pr
    for h in range(heads):
        norm = jnp.sum(nacc[h], axis=0, keepdims=True)
        norm_rows = jnp.where(lax.broadcasted_iota(jnp.int32, (16, hs), 0) == h, norm, 0.0)
        for p in range(NE):
            if p // per_head == h:
                mt[p, 0:pr, :] = macc[h, (p % per_head) * pr : (p % per_head + 1) * pr, :].astype(BF16)
            mt[p, pr : pr + 16, :] += norm_rows.astype(BF16)

    def a_copy(i):
        return remote(mt.at[rem(e + i, NE)], ga.at[e], asend.at[0], arecv.at[0], ee(i))

    def b_copy(d):
        return remote(tb, gb.at[z], bsend.at[d], brecv.at[d], zz(d))

    def c_copy(i):
        return remote(pc.at[rem(e + i, NE)], gc.at[e], csend.at[0], crecv.at[0], ee(i))

    for i in range(1, NE):
        a_copy(i).start()
    ga[e] = mt[e]
    o_pair().start()
    o_cross().start()
    done(wof.at[2, pl.ds(0, (NZ - 1) * br), :], o1r.at[0])
    for i in range(1, NX):
        o_x(i).start()

    done(ga.at[pl.ds(0, NE - 1)], arecv.at[0])
    plane = ga[0].astype(F32)
    for p in range(1, NE):
        plane += ga[p].astype(F32)
    tb[...] = plane.astype(BF16)
    for d in range(1, NZ):

        @pl.when(z + d < NZ)
        def _(d=d):
            b_copy(d).start()

    def put_q(rows, q):
        q = q.astype(BF16)
        for h in range(heads):
            q_s[h, rows, :] = q[:, h * hs : (h + 1) * hs]

    @pl.when(own)
    def _():
        def q_rows(j, carry):
            rows = chunk(j)
            add = jnp.dot(xbuf[rows, block(last)], wbuf[block(last), 2 * gw : 3 * gw], preferred_element_type=F32)
            put_q(rows, acc[rows, 2 * gw : 3 * gw] + add)
            return carry

        lax.fori_loop(0, 4, q_rows, 0)

    @pl.when(other)
    def _():
        done(wbuf.at[pl.ds(0, fs), pl.ds(0, gw)], wcr.at[1])
        done(wbuf.at[pl.ds(0, 2 * NZ * wr), pl.ds(0, gw)], wxr.at[1])
        g_copy().wait_recv()

        def q_rows(j, carry):
            rows = chunk(j)
            put_q(rows, jnp.dot(xbuf[rows, :], wbuf[:, 2 * gw : 3 * gw], preferred_element_type=F32))
            return carry

        lax.fori_loop(0, 4, q_rows, 0)

    shares = [jax.nn.sigmoid(lb[h : h + 1, :]) for h in range(heads)]
    scale = 1.0 / hs**0.5
    lower = lax.broadcasted_iota(jnp.int32, (rc, rc), 1) <= lax.broadcasted_iota(jnp.int32, (rc, rc), 0)

    def attend(h):
        for i in range(4):
            rows = slice(i * rc, (i + 1) * rc)
            q = q_s[h, rows, :]
            diag = lax.dot_general(q, k_s[h, rows, :], NT, preferred_element_type=F32) * scale
            diag = jnp.where(lower, diag, -1e30)
            top = jnp.max(diag, axis=1, keepdims=True)
            if i:
                before = lax.dot_general(q, k_s[h, 0 : i * rc, :], NT, preferred_element_type=F32) * scale
                top = jnp.maximum(top, jnp.max(before, axis=1, keepdims=True))
                pb = jnp.exp(before - top)
            pd = jnp.exp(diag - top)
            total = jnp.sum(pd, axis=1, keepdims=True)
            got = jnp.dot(pd.astype(BF16), v_s[h, rows, :], preferred_element_type=F32)
            if i:
                total += jnp.sum(pb, axis=1, keepdims=True)
                got += jnp.dot(pb.astype(BF16), v_s[h, 0 : i * rc, :], preferred_element_type=F32)
            loc[h, rows, :] = got / total * (1.0 - shares[h])

    attend(0)

    attend(1)

    for d in range(1, NZ):

        @pl.when(z - d >= 0)
        def _(d=d):
            b_copy(d).wait_recv()

    run = lax.fori_loop(0, z, lambda k, s: s + gb[k].astype(F32), jnp.zeros(tb.shape, F32))
    for p in range(NE):
        pc[p] = run.astype(BF16)
        run += ga[p].astype(F32)
    for i in range(1, NE):
        c_copy(i).start()
    gc[e] = pc[e]

    done(gc.at[pl.ds(0, NE - 1)], crecv.at[0])
    for p in range(NE):
        mem[p // per_head, (p % per_head) * pr : (p % per_head + 1) * pr, :] = gc[p, 0:pr, :]

    sizes = [seg // 8] * 7 + [seg // 16] * 2
    spans = [(sum(sizes[:u]), size) for u, size in enumerate(sizes)]

    def m_ref(u, f):
        return mixs.at[pl.ds(*spans[u]), group(f)]

    def m_pair(u, f):
        return remote(m_ref(u, f), m_ref(u, f), psend.at[0], precv.at[u], {"y": part})

    def m_sib(u, f):
        return remote(m_ref(u, f), m_ref(u, f), dsend.at[0], drecv.at[u], sibling)

    def m_on(u, f):
        return remote(m_ref(u, f), m_ref(u, f), fsend.at[0], frecv.at[u], sibling)

    for u in range(NU):
        rows = pl.ds(*spans[u])
        for h in range(heads):
            fq = feature(q_s[h, rows, :].astype(F32)).astype(BF16)
            norm = jnp.broadcast_to(gc[0, pr + h : pr + h + 1, :], (hs, hs))
            denom = lax.dot_general(fq, norm, NT, preferred_element_type=F32)
            numer = jnp.dot(fq, mem[h], preferred_element_type=F32)
            val = shares[h] * (numer / jnp.maximum(denom, 1.0)) + loc[h, rows, :]
            mixs[rows, pl.ds(pl.multiple_of(g * gw + h * hs, hs), hs)] = val.astype(BF16)
        m_pair(u, g).start()
        m_sib(u, g).start()

    def o_copy(u):
        rows = pl.ds(*spans[u])
        dev = {"y": y + c * (cross - y), "c": m}
        return remote(outs.at[rows, :], out.at[rows, :], osend.at[0], orecv.at[0], dev)

    for step in range(NU + 1):
        if step < NU:
            m_pair(step, gp).wait_recv()
            m_on(step, gp).start()
        if step:
            u = step - 1
            if u == 0:
                done(wof.at[2, pl.ds(0, (NX - 1) * NZ * br), :], o2r.at[0])
                done(wof.at[0], o3r.at[0])
                done(wof.at[0], o3r.at[1])
                done(wof.at[0], lsem.at[2])
            rows = pl.ds(*spans[u])
            m_sib(u, NY - 1 - g).wait_recv()
            m_on(u, NY - 1 - gp).wait_recv()
            o = jnp.dot(mixs[rows, group(y)], wof[0], preferred_element_type=F32)
            for r in range(1, NY):
                o += jnp.dot(mixs[rows, group(rem(y + r, NY))], wof[r], preferred_element_type=F32)
            outs[rows, :] = o.astype(BF16)

            @pl.when(at_home)
            def _(rows=rows):
                fetch(outs.at[rows, :], out.at[rows, :], 3)

            @pl.when(jnp.logical_not(at_home))
            def _(u=u):
                o_copy(u).start()

    @pl.when(at_home)
    def _():
        done(outs, lsem.at[3])

    @pl.when(jnp.logical_not(at_home))
    def _():
        done(outs, osend.at[0])

    @pl.when(jnp.logical_not(at_home))
    def _():
        done(outs, orecv.at[0])

    done(outs, psend.at[0])
    done(outs, dsend.at[0])
    done(outs, fsend.at[0])

    @pl.when(is_main)
    def _():
        done(wbuf, tsend.at[0])

    @pl.when(is_helper)
    def _():
        done(xbuf.at[:, pl.ds(0, fs)], tsend.at[0])
        done(wbuf.at[pl.ds(0, fs), :], wcs.at[0])

    @pl.when(other)
    def _():
        done(wbuf.at[pl.ds(0, wr), :], wys.at[0])
        done(wbuf.at[pl.ds(0, (NZ - 1) * wr), :], wzs.at[0])
        done(wbuf.at[pl.ds(0, 2 * NZ * wr), :], wxs.at[0])
        g_copy().wait_send()

    done(wof.at[2, pl.ds(0, br), :], o0s.at[0])
    done(wof.at[2, pl.ds(0, (NZ - 1) * br), :], o1s.at[0])
    done(wof.at[2, pl.ds(0, (NX - 1) * NZ * br), :], o2s.at[0])
    done(wof.at[pl.ds(0, 2)], o3s.at[0])
    done(ga.at[pl.ds(0, NE - 1)], asend.at[0])
    done(gc.at[pl.ds(0, NE - 1)], csend.at[0])
    for d in range(1, NZ):

        @pl.when(z + d < NZ)
        def _(d=d):
            b_copy(d).wait_send()


def on_device(tokens, w_query, w_key, w_value, w_out, mix_logit):
    seg, fs = tokens.shape
    heads = mix_logit.shape[0]
    gw = w_query.shape[1]
    hs = gw // heads
    pr = heads * hs // NE
    hbm = pl.BlockSpec(memory_space=pl.ANY)
    dma = pltpu.SemaphoreType.DMA
    return pl.pallas_call(
        kernel,
        out_shape=jax.ShapeDtypeStruct((seg, fs), BF16),
        in_specs=[hbm] * 5 + [pl.BlockSpec(memory_space=pltpu.SMEM)],
        out_specs=hbm,
        scratch_shapes=[
            pltpu.VMEM((seg, NY * fs), BF16),
            pltpu.VMEM((NY * fs, 3 * gw), BF16),
            pltpu.VMEM((seg, 3 * gw), F32),
            pltpu.VMEM((heads, seg, hs), BF16),
            pltpu.VMEM((heads, seg, hs), BF16),
            pltpu.VMEM((heads, seg, hs), BF16),
            pltpu.VMEM((heads, seg, hs), F32),
            pltpu.VMEM((NY, gw, fs), BF16),
            pltpu.VMEM((heads, hs, hs), F32),
            pltpu.VMEM((heads, 8, hs), F32),
            pltpu.VMEM((NE, pr + 16, hs), BF16),
            pltpu.VMEM((NE, pr + 16, hs), BF16),
            pltpu.VMEM((pr + 16, hs), BF16),
            pltpu.VMEM((NZ, pr + 16, hs), BF16),
            pltpu.VMEM((NE, pr + 16, hs), BF16),
            pltpu.VMEM((NE, pr + 16, hs), BF16),
            pltpu.VMEM((heads, hs, hs), BF16),
            pltpu.VMEM((seg, NY * gw), BF16),
            pltpu.VMEM((seg, fs), BF16),
            pltpu.VMEM((8, hs), F32),
            pltpu.VMEM((8, hs), F32),
            dma((4,)),
            dma((1,)), dma((4, 4)),
            dma((1,)), dma((2,)),
            dma((1,)), dma((2, NZ)),
            dma((1,)), dma((2,)),
            dma((1,)), dma((2,)),
            dma((1,)), dma((1,)),
            dma((1,)), dma((1,)),
            dma((1,)), dma((1,)),
            dma((1,)), dma((2,)),
            dma((1,)), dma((1,)),
            dma((1,)), dma((1,)),
            dma((NZ,)), dma((NZ,)),
            dma((1,)), dma((1,)),
            dma((1,)), dma((NU,)),
            dma((1,)), dma((NU,)),
            dma((1,)), dma((NU,)),
            dma((1,)), dma((1,)),
        ],
        compiler_params=pltpu.CompilerParams(
            collective_id=0, has_side_effects=True, vmem_limit_bytes=52 * 2**20
        ),
    )(tokens, w_query, w_key, w_value, w_out, mix_logit)


def solution(mesh):
    torus = Mesh(mesh.devices.reshape(NZ, NX, NC, NY), ("z", "x", "c", "y"))
    return jax.shard_map(
        on_device,
        mesh=torus,
        in_specs=(P(SEQ, "y"), P(None, "y"), P(None, "y"), P(None, "y"), P("y", None), P("y")),
        out_specs=P(SEQ, "y"),
        check_vma=False,
    )
```

```python
import functools

import jax
import jax.numpy as jnp
from jax import lax
from jax.experimental import pallas as pl
from jax.experimental.pallas import tpu as pltpu
from jax.sharding import Mesh
from jax.sharding import PartitionSpec as P

SEQ = ("z", "x", "c")
MESH = pl.DeviceIdType.MESH
F32, BF16 = jnp.float32, jnp.bfloat16
NZ, NX, NC, NY = 8, 4, 2, 4
NE = NX * NC
NU = 9
ZORDER = (1, 7, 2, 6, 3, 5, 4)
NT = (((1,), (1,)), ((), ()))
TN = (((0,), (0,)), ((), ()))


def feature(values):
    return jnp.where(values > 0, values + 1.0, jnp.exp(values))


def kernel(
    tok, wq, wk, wv, wo, logit, out,
    xbuf, wbuf, acc, q_s, k_s, v_s, loc, wof, macc, nacc, mt, ga, tb, gb, pc, gc, mem, nrm, mixs, outs, ls, lb,
    lsem, tsend, trecv, wys, wyr, wzs, wzr, wqr, wxs, wxr, wcs, wcr, o0s, o0r, o1s, o1r, o2s, o2r, o3s, o3r, gsend, grecv,
    asend, arecv, bsend, brecv, csend, crecv, psend, precv, dsend, drecv, fsend, osend, orecv,
):
    z, x, c, y = (lax.axis_index(a) for a in ("z", "x", "c", "y"))
    rem, div = lax.rem, lax.div
    m = div(y, 2)
    part = y + 1 - 2 * rem(y, 2)
    cross = NY - 1 - y
    g = y + c * (cross - y)
    gp = g + 1 - 2 * rem(g, 2)
    e = x * NC + m
    seg, fs = tok.shape
    heads, _, hs = q_s.shape
    rc = seg // 4
    gw = heads * hs
    pr = heads * hs // NE
    br = gw // (NZ * NX)
    wr = NY * fs // (NZ * NX)
    is_source, not_source = c == m, c != m
    is_main = c == 1
    at_home = c + m == 0

    def yy(r):
        return {"y": rem(y + r, NY)}

    def zz(d):
        return {"z": rem(z + d, NZ)}

    def xx(i):
        return {"x": rem(x + i, NX)}

    def ee(i):
        o = rem(e + i, NE)
        par = rem(o, NC)
        diff = par + m - 2 * par * m
        return {"x": div(o, NC), "y": y + diff * (cross - y)}

    sibling = {"c": 1 - c}

    def remote(src, dst, ssem, rsem, dev):
        return pltpu.make_async_remote_copy(
            src_ref=src, dst_ref=dst, send_sem=ssem, recv_sem=rsem, device_id=dev, device_id_type=MESH
        )

    def fetch(src, dst, k):
        pltpu.make_async_copy(src, dst, lsem.at[k]).start()

    def done(ref, sem):
        pltpu.make_async_copy(ref, ref, sem).wait()

    def chunk(j):
        return pl.ds(pl.multiple_of(j * rc, rc), rc)

    def block(f):
        return pl.ds(pl.multiple_of(f * fs, fs), fs)

    def group(f):
        return pl.ds(pl.multiple_of(f * gw, gw), gw)

    barrier = pltpu.get_barrier_semaphore()
    peers = [zz(d) for d in range(1, NZ)] + [yy(r) for r in range(1, NY)] + [xx(i) for i in range(1, NX)]
    peers += [{"x": rem(x + i, NX), "y": cross} for i in range(1, NX)] + [sibling, {"y": cross, "c": 1 - c}, {"y": part, "c": 1 - c}]
    for dev in peers:
        pl.semaphore_signal(barrier, inc=1, device_id=dev, device_id_type=MESH)

    ls[...] = jnp.full(ls.shape, logit[c], F32)

    weights = (wk, wv, wq)
    nh = 3 * hs
    ok, oq = slice(0, 2 * hs), slice(2 * hs, nh)
    ck, cq = slice(nh, nh + 2 * hs), slice(nh + 2 * hs, 2 * nh)

    def head(ct):
        return pl.ds(pl.multiple_of(ct * hs, hs), hs)

    @pl.when(is_source)
    def _():
        fetch(tok, xbuf.at[:, block(y)], 0)

    for i, w in enumerate(weights):
        fetch(w.at[:, head(c)], wbuf.at[:, pl.ds(i * hs, hs)], 1)

    fetch(wo.at[:, group(g)], wof.at[0], 2)

    pl.semaphore_wait(barrier, len(peers))

    def t_pair(k):
        return remote(
            tok.at[chunk(k), :], xbuf.at[chunk(k), block(y)], tsend.at[0], trecv.at[0, k], {"y": part, "c": 1}
        )

    def t_cross(k):
        return remote(
            tok.at[chunk(k), :], xbuf.at[chunk(k), block(y)], tsend.at[0], trecv.at[0, k], {"y": cross, "c": 1}
        )

    def t_on(k):
        ref = xbuf.at[chunk(k), block(cross)]
        return remote(ref, ref, tsend.at[1], trecv.at[1, k], {"y": part})

    def t_sib(k, kind, f):
        ref = xbuf.at[chunk(k), block(f)]
        return remote(ref, ref, tsend.at[1], trecv.at[kind, k], sibling)

    def t_own():
        return remote(tok, xbuf.at[:, block(y)], tsend.at[0], trecv.at[2, 0], sibling)

    def t_wait(k, kind, f):
        t_sib(k, kind, f).wait_recv()

    def w_rows(xp, zp):
        return pl.ds(pl.multiple_of((xp * NZ + zp) * wr, wr), wr)

    far_block = rem(x + 2, NX)
    w_cols = (pl.ds(nh, 2 * hs), pl.ds(nh + 2 * hs, hs), pl.ds(nh + hs, hs))

    def w_piece(i):
        return remote(
            weights[i].at[w_rows(x, z), head(c)], wbuf.at[w_rows(x, z), pl.ds(nh + i * hs, hs)],
            wys.at[0], wyr.at[i // 2], {"y": cross},
        )

    def w_z(kind, d):
        ref = wbuf.at[w_rows(x, z), w_cols[kind]]
        return remote(ref, ref, wzs.at[0], wqr.at[0] if kind else wzr.at[d], zz(d))

    def w_x(kind, i, d):
        ref = wbuf.at[w_rows(x, rem(z + NZ - d, NZ)), w_cols[kind]]
        return remote(ref, ref, wxs.at[kind], wxr.at[kind], xx(i))

    def w_xs(d):
        w_x(0, 1, d).start()
        w_x(0, 3, d).start()
        w_x(2, 2, d).start()

    def w_cross(i, ct):
        return remote(
            weights[i].at[block(far_block), head(ct)], wbuf.at[block(far_block), pl.ds(nh + i * hs, hs)],
            wcs.at[0], wcr.at[i // 2], {"y": cross, "c": ct},
        )

    def o_rows(xp, zp):
        return pl.ds(pl.multiple_of((xp * NZ + zp) * br, br), br)

    def o_y():
        return remote(
            wo.at[o_rows(x, z), group(NY - 1 - gp)], wof.at[2, o_rows(x, z), :], o0s.at[0], o0r.at[0], yy(2)
        )

    def o_z(d):
        ref = wof.at[2, o_rows(x, z), :]
        return remote(ref, ref, o1s.at[0], o1r.at[0], zz(d))

    def o_x(i):
        ref = wof.at[2, pl.ds(pl.multiple_of(x * NZ * br, NZ * br), NZ * br), :]
        return remote(ref, ref, o2s.at[0], o2r.at[0], xx(i))

    def o_pair():
        return remote(
            wo.at[:, group(gp)], wof.at[3 - 2 * rem(y, 2)], o3s.at[0], o3r.at[0], {"y": part}
        )

    def o_cross():
        return remote(
            wo.at[:, group(NY - 1 - g)], wof.at[1 + 2 * rem(y, 2)], o3s.at[0], o3r.at[1], {"y": cross}
        )

    def g_copy():
        return remote(ls, lb, gsend.at[0], grecv.at[0], {"y": cross})

    for i in range(2):
        w_piece(i).start()
    o_y().start()

    @pl.when(is_source)
    def _():
        for k in range(4):
            t_pair(k).start()
        t_own().start()

    @pl.when(not_source)
    def _():
        for k in range(4):
            t_cross(k).start()

    w_piece(2).start()
    g_copy().start()

    @pl.when(not_source)
    def _():
        for i in (0, 2):
            for ct in (1, 0):
                w_cross(i, ct).start()
        o_cross().start()

    macc[...] = jnp.zeros_like(macc)
    nacc[...] = jnp.zeros_like(nacc)

    @pl.when(is_source)
    def _():
        done(xbuf.at[:, block(y)], lsem.at[0])

    @pl.when(not_source)
    def _():
        t_own().wait_recv()

    done(wbuf.at[:, pl.ds(0, nh)], lsem.at[1])

    def own_dot(j, carry):
        acc[chunk(j), 0:nh] = jnp.dot(
            xbuf[chunk(j), block(y)], wbuf[block(y), 0:nh], preferred_element_type=F32
        )
        return carry

    lax.fori_loop(0, 2, own_dot, 0)
    done(wbuf.at[pl.ds(0, wr), pl.ds(0, 2 * hs)], wyr.at[0])
    for d in ZORDER:
        w_z(0, d).start()
    w_xs(0)
    lax.fori_loop(2, 4, own_dot, 0)

    forward_at = {0: (1, 7), 1: (2, 6), 2: (3, 5), 3: (4,)}
    for k in range(4):
        done(xbuf.at[chunk(k), pl.ds(0, 2 * fs)], trecv.at[0, k])

        @pl.when(is_main)
        def _(k=k):
            t_on(k).start()
            t_sib(k, 0, cross).start()
            t_sib(k, 0, part).start()

        for d in forward_at[k]:
            w_z(0, d).wait_recv()
            w_xs(d)
        rows = chunk(k)
        add = jnp.dot(xbuf[rows, block(part)], wbuf[block(part), 0:nh], preferred_element_type=F32)
        add += jnp.dot(xbuf[rows, block(cross)], wbuf[block(cross), 0:nh], preferred_element_type=F32)
        acc[rows, 0:nh] += add

    def finish(h, rows, kv):
        kv = kv.astype(BF16)
        key, val = kv[:, :hs], kv[:, hs:]
        k_s[h, rows, :] = key
        v_s[h, rows, :] = val
        fk = feature(key.astype(F32)).astype(BF16)
        macc[h] += lax.dot_general(fk, val, TN, preferred_element_type=F32)
        nacc[h] += jnp.sum(fk.astype(F32).reshape(rc // 8, 8, hs), axis=0)

    def cross_rows(j):
        rows = chunk(j)
        kv = acc[rows, ck]
        for i in range(1, NX):
            f = block(rem(x + i, NX))
            kv += jnp.dot(xbuf[rows, f], wbuf[f, ck], preferred_element_type=F32)
        finish(1, rows, kv)

    done(wbuf.at[pl.ds(0, wr), pl.ds(0, hs)], wyr.at[1])
    for d in ZORDER:
        w_z(1, d).start()
    w_x(1, 1, 0).start()
    w_x(1, 3, 0).start()

    done(wof.at[2, pl.ds(0, br), :], o0r.at[0])
    for d in ZORDER:
        o_z(d).start()

    def q_forward():
        done(wbuf.at[pl.ds(0, wr * (NZ - 1)), pl.ds(0, hs)], wqr.at[0])
        for d in ZORDER:
            w_x(1, 1, d).start()
            w_x(1, 3, d).start()

    last = NY - 1 - part
    for k in range(4):
        if k == 3:
            done(wbuf.at[pl.ds(0, 2 * NZ * wr), pl.ds(0, 2 * hs)], wxr.at[0])
            done(wbuf.at[pl.ds(0, fs), pl.ds(0, hs)], wxr.at[2])
            done(wbuf.at[pl.ds(0, fs), pl.ds(0, hs)], wcr.at[0])

            for j in range(3):
                cross_rows(j)
            pl.when(c == 1)(q_forward)

        t_wait(k, 1, last)

        @pl.when(is_main)
        def _(k=k):
            t_sib(k, 1, last).start()

        rows = chunk(k)
        acc[rows, ck] = jnp.dot(xbuf[rows, block(x)], wbuf[block(x), ck], preferred_element_type=F32)
        add = jnp.dot(xbuf[rows, block(last)], wbuf[block(last), ok], preferred_element_type=F32)
        finish(0, rows, acc[rows, ok] + add)

    cross_rows(3)

    per_head, hw = hs // pr, hs // 2
    norms = []
    for h in range(heads):
        slot = m if h == 0 else 1 - m
        norm = jnp.sum(nacc[h], axis=0, keepdims=True)
        which = lax.broadcasted_iota(jnp.int32, (16, hw), 0)
        norms += [jnp.where(which == 2 * slot + i, norm[:, i * hw : (i + 1) * hw], 0.0) for i in range(2)]
        for p in range(per_head):
            rows = slice(p * pr, (p + 1) * pr)
            for i in range(2):
                mt[slot * per_head + p, i * pr : (i + 1) * pr, :] = macc[h, rows, i * hw : (i + 1) * hw].astype(BF16)
    for p in range(NE):
        mt[p, 2 * pr :, :] = sum(norms).astype(BF16)

    def a_copy(i):
        return remote(mt.at[rem(e + i, NE)], ga.at[e], asend.at[0], arecv.at[0], ee(i))

    def b_copy(d):
        return remote(tb, gb.at[z], bsend.at[0], brecv.at[0], zz(d))

    def c_copy(i):
        return remote(pc.at[rem(e + i, NE)], gc.at[e], csend.at[0], crecv.at[0], ee(i))

    for i in range(1, NE):
        a_copy(i).start()
    ga[e] = mt[e]
    o_pair().start()
    pl.when(c == 0)(q_forward)

    scale = 1.0 / hs**0.5
    lower = lax.broadcasted_iota(jnp.int32, (rc, rc), 1) <= lax.broadcasted_iota(jnp.int32, (rc, rc), 0)

    def attend(h):
        for i in range(4):
            rows = slice(i * rc, (i + 1) * rc)
            q = q_s[h, rows, :]
            diag = lax.dot_general(q, k_s[h, rows, :], NT, preferred_element_type=F32) * scale
            diag = jnp.where(lower, diag, -1e30)
            top = jnp.max(diag, axis=1, keepdims=True)
            if i:
                before = lax.dot_general(q, k_s[h, 0 : i * rc, :], NT, preferred_element_type=F32) * scale
                top = jnp.maximum(top, jnp.max(before, axis=1, keepdims=True))
                pb = jnp.exp(before - top)
            pd = jnp.exp(diag - top)
            total = jnp.sum(pd, axis=1, keepdims=True)
            got = jnp.dot(pd.astype(BF16), v_s[h, rows, :], preferred_element_type=F32)
            if i:
                total += jnp.sum(pb, axis=1, keepdims=True)
                got += jnp.dot(pb.astype(BF16), v_s[h, 0 : i * rc, :], preferred_element_type=F32)
            loc[h, rows, :] = got / total * (1.0 - shares[h])

    def own_q(j, carry):
        rows = chunk(j)
        add = jnp.dot(xbuf[rows, block(last)], wbuf[block(last), oq], preferred_element_type=F32)
        q_s[0, rows, :] = (acc[rows, oq] + add).astype(BF16)
        return carry

    lax.fori_loop(0, 4, own_q, 0)
    shares = [jax.nn.sigmoid(ls[0:1, :])]
    attend(0)

    done(ga.at[pl.ds(0, NE - 1)], arecv.at[0])
    plane = ga[0].astype(F32)
    for p in range(1, NE):
        plane += ga[p].astype(F32)
    tb[...] = plane.astype(BF16)
    for d in (4, 3, 5, 2, 6, 1, 7):

        @pl.when(z + d < NZ)
        def _(d=d):
            b_copy(d).start()

    def bulk():
        @pl.when(is_source)
        def _():
            o_cross().start()

        for i in range(1, NX):
            o_x(i).start()

    done(wof.at[2, pl.ds(0, (NZ - 1) * br), :], o1r.at[0])
    pl.when(c == 0)(bulk)

    done(wbuf.at[pl.ds(0, fs), pl.ds(0, hs)], wcr.at[1])
    done(wbuf.at[pl.ds(0, 2 * NZ * wr), pl.ds(0, hs)], wxr.at[1])
    g_copy().wait_recv()

    def cross_q(j, carry):
        rows = chunk(j)
        q_s[1, rows, :] = jnp.dot(xbuf[rows, :], wbuf[:, cq], preferred_element_type=F32).astype(BF16)
        return carry

    lax.fori_loop(0, 4, cross_q, 0)
    shares.append(jax.nn.sigmoid(lb[0:1, :]))

    attend(1)

    for n in range(1, NZ):

        @pl.when(z == n)
        def _(n=n):
            done(gb.at[pl.ds(0, n)], brecv.at[0])

    run = lax.fori_loop(0, z, lambda k, s: s + gb[k].astype(F32), jnp.zeros(tb.shape, F32))
    for p in range(NE):
        pc[p] = run.astype(BF16)
        run += ga[p].astype(F32)
    for i in range(1, NE):
        c_copy(i).start()
    gc[e] = pc[e]
    pl.when(c == 1)(bulk)

    done(gc.at[pl.ds(0, NE - 1)], crecv.at[0])
    for h in range(heads):
        slot = m if h == 0 else 1 - m
        for p in range(per_head):
            for i in range(2):
                mem[h, p * pr : (p + 1) * pr, i * hw : (i + 1) * hw] = gc[slot * per_head + p, i * pr : (i + 1) * pr, :]
        for i in range(2):
            row = 2 * pr + i
            norm = jnp.where(slot == 0, gc[0, row : row + 1, :].astype(F32), gc[0, row + 2 : row + 3, :].astype(F32))
            nrm[h, :, i * hw : (i + 1) * hw] = jnp.broadcast_to(norm, (hs, hw)).astype(BF16)

    sizes = [seg // 8] * 7 + [seg // 16] * 2
    spans = [(sum(sizes[:u]), size) for u, size in enumerate(sizes)]

    pidx = div(y * cross, 2)

    def m_ref(u, cc, pp):
        return mixs.at[pl.ds(*spans[u]), pl.ds(pl.multiple_of(cc * 4 * hs + pp * 2 * hs, hs), 2 * hs)]

    def m_pair(u, pp):
        return remote(m_ref(u, c, pp), m_ref(u, c, pp), psend.at[0], precv.at[u], {"y": part})

    def m_sib(u, pp, fin):
        return remote(m_ref(u, c, pp), m_ref(u, c, pp), fin.at[0], drecv.at[u], sibling)

    for u in range(NU):
        rows = pl.ds(*spans[u])
        for h in range(heads):
            fq = feature(q_s[h, rows, :].astype(F32)).astype(BF16)
            denom = lax.dot_general(fq, nrm[h], NT, preferred_element_type=F32)
            numer = jnp.dot(fq, mem[h], preferred_element_type=F32)
            val = shares[h] * (numer / jnp.maximum(denom, 1.0)) + loc[h, rows, :]
            at = c * 4 * hs + pidx * 2 * hs + (m if h == 0 else 1 - m) * hs
            mixs[rows, pl.ds(pl.multiple_of(at, hs), hs)] = val.astype(BF16)
        m_pair(u, pidx).start()
        m_sib(u, pidx, dsend).start()

    def o_copy(u):
        rows = pl.ds(*spans[u])
        dev = {"y": y + c * (cross - y), "c": m}
        return remote(outs.at[rows, :], out.at[rows, :], osend.at[0], orecv.at[0], dev)

    for step in range(NU + 1):
        if step < NU:
            m_pair(step, 1 - pidx).wait_recv()
            m_sib(step, 1 - pidx, fsend).start()
        if step:
            u = step - 1
            if u == 0:
                done(wof.at[2, pl.ds(0, (NX - 1) * NZ * br), :], o2r.at[0])
                done(wof.at[0], o3r.at[0])
                done(wof.at[0], o3r.at[1])
                done(wof.at[0], lsem.at[2])
            rows = pl.ds(*spans[u])
            done(mixs.at[rows, pl.ds(0, 2 * gw)], drecv.at[u])
            o = jnp.zeros((spans[u][1], fs), F32)
            for cc in range(NC):
                for pos, grp in enumerate((0, 3, 1, 2)):
                    at = cc * 4 * hs + pos * hs
                    part_w = wof[rem(grp + NY - y, NY), cc * hs : (cc + 1) * hs, :]
                    o += jnp.dot(mixs[rows, at : at + hs], part_w, preferred_element_type=F32)
            outs[rows, :] = o.astype(BF16)

            @pl.when(at_home)
            def _(rows=rows):
                fetch(outs.at[rows, :], out.at[rows, :], 3)

            @pl.when(jnp.logical_not(at_home))
            def _(u=u):
                o_copy(u).start()

    @pl.when(at_home)
    def _():
        done(outs, lsem.at[3])

    @pl.when(jnp.logical_not(at_home))
    def _():
        done(outs, osend.at[0])

    @pl.when(jnp.logical_not(at_home))
    def _():
        done(outs, orecv.at[0])

    done(outs, psend.at[0])
    done(outs, dsend.at[0])
    done(outs, fsend.at[0])

    @pl.when(is_source)
    def _():
        done(xbuf.at[:, pl.ds(0, 2 * fs)], tsend.at[0])

    @pl.when(is_main)
    def _():
        done(xbuf, tsend.at[1])

    @pl.when(not_source)
    def _():
        done(xbuf.at[:, pl.ds(0, fs)], tsend.at[0])
        done(wbuf.at[pl.ds(0, fs), pl.ds(0, 2 * gw)], wcs.at[0])

    done(wbuf.at[pl.ds(0, wr), pl.ds(0, nh)], wys.at[0])
    done(wbuf.at[pl.ds(0, (NZ - 1) * wr), pl.ds(0, nh)], wzs.at[0])
    done(wbuf.at[pl.ds(0, 2 * NZ * wr), pl.ds(0, 2 * hs)], wxs.at[0])
    done(wbuf.at[pl.ds(0, 2 * NZ * wr), pl.ds(0, hs)], wxs.at[1])
    done(wbuf.at[pl.ds(0, fs), pl.ds(0, hs)], wxs.at[2])
    g_copy().wait_send()

    done(wof.at[2, pl.ds(0, br), :], o0s.at[0])
    done(wof.at[2, pl.ds(0, (NZ - 1) * br), :], o1s.at[0])
    done(wof.at[2, pl.ds(0, (NX - 1) * NZ * br), :], o2s.at[0])
    done(wof.at[pl.ds(0, 2)], o3s.at[0])
    done(ga.at[pl.ds(0, NE - 1)], asend.at[0])
    done(gc.at[pl.ds(0, NE - 1)], csend.at[0])
    for n in range(1, NZ):

        @pl.when(z == NZ - 1 - n)
        def _(n=n):
            done(gb.at[pl.ds(0, n)], bsend.at[0])


def on_device(tokens, w_query, w_key, w_value, w_out, mix_logit):
    seg, fs = tokens.shape
    heads = mix_logit.shape[0]
    gw = w_query.shape[1]
    hs = gw // heads
    pr = heads * hs // NE
    hbm = pl.BlockSpec(memory_space=pl.ANY)
    dma = pltpu.SemaphoreType.DMA
    return pl.pallas_call(
        kernel,
        out_shape=jax.ShapeDtypeStruct((seg, fs), BF16),
        in_specs=[hbm] * 5 + [pl.BlockSpec(memory_space=pltpu.SMEM)],
        out_specs=hbm,
        scratch_shapes=[
            pltpu.VMEM((seg, NY * fs), BF16),
            pltpu.VMEM((NY * fs, 3 * gw), BF16),
            pltpu.VMEM((seg, 3 * gw), F32),
            pltpu.VMEM((heads, seg, hs), BF16),
            pltpu.VMEM((heads, seg, hs), BF16),
            pltpu.VMEM((heads, seg, hs), BF16),
            pltpu.VMEM((heads, seg, hs), F32),
            pltpu.VMEM((NY, gw, fs), BF16),
            pltpu.VMEM((heads, hs, hs), F32),
            pltpu.VMEM((heads, 8, hs), F32),
            pltpu.VMEM((NE, 2 * pr + 16, hs // 2), BF16),
            pltpu.VMEM((NE, 2 * pr + 16, hs // 2), BF16),
            pltpu.VMEM((2 * pr + 16, hs // 2), BF16),
            pltpu.VMEM((NZ, 2 * pr + 16, hs // 2), BF16),
            pltpu.VMEM((NE, 2 * pr + 16, hs // 2), BF16),
            pltpu.VMEM((NE, 2 * pr + 16, hs // 2), BF16),
            pltpu.VMEM((heads, hs, hs), BF16),
            pltpu.VMEM((heads, hs, hs), BF16),
            pltpu.VMEM((seg, NY * gw), BF16),
            pltpu.VMEM((seg, fs), BF16),
            pltpu.VMEM((8, hs), F32),
            pltpu.VMEM((8, hs), F32),
            dma((4,)),
            dma((2,)), dma((3, 4)),
            dma((1,)), dma((2,)),
            dma((1,)), dma((NZ,)), dma((1,)),
            dma((3,)), dma((3,)),
            dma((1,)), dma((2,)),
            dma((1,)), dma((1,)),
            dma((1,)), dma((1,)),
            dma((1,)), dma((1,)),
            dma((1,)), dma((2,)),
            dma((1,)), dma((1,)),
            dma((1,)), dma((1,)),
            dma((1,)), dma((1,)),
            dma((1,)), dma((1,)),
            dma((1,)), dma((NU,)),
            dma((1,)), dma((NU,)),
            dma((1,)),
            dma((1,)), dma((1,)),
        ],
        compiler_params=pltpu.CompilerParams(
            collective_id=0, has_side_effects=True, vmem_limit_bytes=52 * 2**20
        ),
    )(tokens, w_query, w_key, w_value, w_out, mix_logit)


def solution(mesh):
    torus = Mesh(mesh.devices.reshape(NZ, NX, NC, NY), ("z", "x", "c", "y"))
    return jax.shard_map(
        on_device,
        mesh=torus,
        in_specs=(P(SEQ, "y"), P(None, "y"), P(None, "y"), P(None, "y"), P("y", None), P("y")),
        out_specs=P(SEQ, "y"),
        check_vma=False,
    )
```

```python
import functools

import jax
import jax.numpy as jnp
from jax import lax
from jax.experimental import pallas as pl
from jax.experimental.pallas import tpu as pltpu
from jax.sharding import Mesh
from jax.sharding import PartitionSpec as P

SEQ = ("z", "x", "c")
MESH = pl.DeviceIdType.MESH
F32, BF16 = jnp.float32, jnp.bfloat16
NZ, NX, NC, NY = 8, 4, 2, 4
NE = NX * NC
NU = 9
ZORDER = (1, 7, 2, 6, 3, 5, 4)
NT = (((1,), (1,)), ((), ()))
TN = (((0,), (0,)), ((), ()))


def feature(values):
    return jnp.where(values > 0, values + 1.0, jnp.exp(values))


def kernel(
    tok, wq, wk, wv, wo, logit, out,
    xbuf, wbuf, acc, q_s, k_s, v_s, loc, wof, macc, nacc, mt, ga, tb, gb, pc, gc, mem, nrm, mixs, outs, ls, lb,
    lsem, tsend, trecv, wys, wyr, wzs, wzr, wqr, wxs, wxr, wcs, wcr, o0s, o0r, o1s, o1r, o2s, o2r, o3s, o3r, gsend, grecv,
    asend, arecv, bsend, brecv, csend, crecv, psend, precv, dsend, drecv, fsend, osend, orecv,
):
    z, x, c, y = (lax.axis_index(a) for a in ("z", "x", "c", "y"))
    rem, div = lax.rem, lax.div
    m = div(y, 2)
    part = y + 1 - 2 * rem(y, 2)
    cross = NY - 1 - y
    g = y + c * (cross - y)
    gp = g + 1 - 2 * rem(g, 2)
    e = x * NC + m
    seg, fs = tok.shape
    heads, _, hs = q_s.shape
    rc = seg // 4
    gw = heads * hs
    pr = heads * hs // NE
    br = gw // (NZ * NX)
    wr = NY * fs // (NZ * NX)
    is_source, not_source = c == m, c != m
    is_main = c == 1
    at_home = c + m == 0

    def yy(r):
        return {"y": rem(y + r, NY)}

    def zz(d):
        return {"z": rem(z + d, NZ)}

    def xx(i):
        return {"x": rem(x + i, NX)}

    def ee(i):
        o = rem(e + i, NE)
        par = rem(o, NC)
        diff = par + m - 2 * par * m
        return {"x": div(o, NC), "y": y + diff * (cross - y)}

    sibling = {"c": 1 - c}

    def remote(src, dst, ssem, rsem, dev):
        return pltpu.make_async_remote_copy(
            src_ref=src, dst_ref=dst, send_sem=ssem, recv_sem=rsem, device_id=dev, device_id_type=MESH
        )

    def fetch(src, dst, k):
        pltpu.make_async_copy(src, dst, lsem.at[k]).start()

    def done(ref, sem):
        pltpu.make_async_copy(ref, ref, sem).wait()

    def chunk(j):
        return pl.ds(pl.multiple_of(j * rc, rc), rc)

    def block(f):
        return pl.ds(pl.multiple_of(f * fs, fs), fs)

    def group(f):
        return pl.ds(pl.multiple_of(f * gw, gw), gw)

    barrier = pltpu.get_barrier_semaphore()
    peers = [zz(d) for d in range(1, NZ)] + [yy(r) for r in range(1, NY)] + [xx(i) for i in range(1, NX)]
    peers += [{"x": rem(x + i, NX), "y": cross} for i in range(1, NX)] + [sibling, {"y": cross, "c": 1 - c}, {"y": part, "c": 1 - c}]
    for dev in peers:
        pl.semaphore_signal(barrier, inc=1, device_id=dev, device_id_type=MESH)

    ls[...] = jnp.full(ls.shape, logit[c], F32)

    weights = (wk, wv, wq)
    nh = 3 * hs
    ok, oq = slice(0, 2 * hs), slice(2 * hs, nh)
    ck, cq = slice(nh, nh + 2 * hs), slice(nh + 2 * hs, 2 * nh)

    def head(ct):
        return pl.ds(pl.multiple_of(ct * hs, hs), hs)

    @pl.when(is_source)
    def _():
        fetch(tok, xbuf.at[:, block(y)], 0)

    for i, w in enumerate(weights):
        fetch(w.at[:, head(c)], wbuf.at[:, pl.ds(i * hs, hs)], 1)

    fetch(wo.at[:, group(g)], wof.at[0], 2)

    pl.semaphore_wait(barrier, len(peers))

    def t_pair(k):
        return remote(
            tok.at[chunk(k), :], xbuf.at[chunk(k), block(y)], tsend.at[0], trecv.at[0, k], {"y": part, "c": 1}
        )

    def t_cross(k):
        return remote(
            tok.at[chunk(k), :], xbuf.at[chunk(k), block(y)], tsend.at[0], trecv.at[3, k], {"y": cross, "c": 1}
        )

    def t_on(k):
        ref = xbuf.at[chunk(k), block(cross)]
        return remote(ref, ref, tsend.at[1], trecv.at[1, k], {"y": part})

    def t_sib(k, kind, f):
        ref = xbuf.at[chunk(k), block(f)]
        return remote(ref, ref, tsend.at[1], trecv.at[kind, k], sibling)

    def t_own():
        return remote(tok, xbuf.at[:, block(y)], tsend.at[0], trecv.at[2, 0], sibling)

    def t_wait(k, kind, f):
        t_sib(k, kind, f).wait_recv()

    def w_rows(xp, zp):
        return pl.ds(pl.multiple_of((xp * NZ + zp) * wr, wr), wr)

    far_block = rem(x + 2, NX)
    w_cols = (pl.ds(nh, 2 * hs), pl.ds(nh + 2 * hs, hs), pl.ds(nh + hs, hs))

    def w_piece(i):
        return remote(
            weights[i].at[w_rows(x, z), head(c)], wbuf.at[w_rows(x, z), pl.ds(nh + i * hs, hs)],
            wys.at[0], wyr.at[i // 2], {"y": cross},
        )

    def w_z(kind, d):
        ref = wbuf.at[w_rows(x, z), w_cols[kind]]
        return remote(ref, ref, wzs.at[0], wqr.at[0] if kind else wzr.at[d], zz(d))

    def w_x(kind, i, d):
        ref = wbuf.at[w_rows(x, rem(z + NZ - d, NZ)), w_cols[kind]]
        return remote(ref, ref, wxs.at[kind], wxr.at[kind], xx(i))

    def w_xs(d):
        w_x(0, 1, d).start()
        w_x(0, 3, d).start()
        w_x(2, 2, d).start()

    def w_cross(i, ct):
        return remote(
            weights[i].at[block(far_block), head(ct)], wbuf.at[block(far_block), pl.ds(nh + i * hs, hs)],
            wcs.at[0], wcr.at[i // 2], {"y": cross, "c": ct},
        )

    def o_rows(xp, zp):
        return pl.ds(pl.multiple_of((xp * NZ + zp) * br, br), br)

    def o_y():
        return remote(
            wo.at[o_rows(x, z), group(NY - 1 - gp)], wof.at[2, o_rows(x, z), :], o0s.at[0], o0r.at[0], yy(2)
        )

    def o_z(d):
        ref = wof.at[2, o_rows(x, z), :]
        return remote(ref, ref, o1s.at[0], o1r.at[0], zz(d))

    def o_x(i):
        ref = wof.at[2, pl.ds(pl.multiple_of(x * NZ * br, NZ * br), NZ * br), :]
        return remote(ref, ref, o2s.at[0], o2r.at[0], xx(i))

    def o_pair():
        return remote(
            wo.at[:, group(gp)], wof.at[3 - 2 * rem(y, 2)], o3s.at[0], o3r.at[0], {"y": part}
        )

    def o_cross():
        return remote(
            wo.at[:, group(NY - 1 - g)], wof.at[1 + 2 * rem(y, 2)], o3s.at[0], o3r.at[1], {"y": cross}
        )

    def g_copy():
        return remote(ls, lb, gsend.at[0], grecv.at[0], {"y": cross})

    for i in range(2):
        w_piece(i).start()
    o_y().start()

    @pl.when(is_source)
    def _():
        for k in range(4):
            t_pair(k).start()
        t_own().start()

    @pl.when(not_source)
    def _():
        for k in range(4):
            t_cross(k).start()

    w_piece(2).start()
    g_copy().start()

    @pl.when(not_source)
    def _():
        for i in (0, 2):
            for ct in (1, 0):
                w_cross(i, ct).start()

    macc[...] = jnp.zeros_like(macc)
    nacc[...] = jnp.zeros_like(nacc)

    @pl.when(is_source)
    def _():
        done(xbuf.at[:, block(y)], lsem.at[0])

    @pl.when(not_source)
    def _():
        t_own().wait_recv()

    done(wbuf.at[:, pl.ds(0, nh)], lsem.at[1])

    def own_dot(j, carry):
        acc[chunk(j), 0:nh] = jnp.dot(
            xbuf[chunk(j), block(y)], wbuf[block(y), 0:nh], preferred_element_type=F32
        )
        return carry

    lax.fori_loop(0, 2, own_dot, 0)
    done(wbuf.at[pl.ds(0, wr), pl.ds(0, 2 * hs)], wyr.at[0])
    for d in ZORDER:
        w_z(0, d).start()
    w_xs(0)
    lax.fori_loop(2, 4, own_dot, 0)

    forward_at = {0: (1, 7), 1: (2, 6), 2: (3, 5), 3: (4,)}
    for k in range(4):
        t_wait(k, 3, cross)

        @pl.when(is_main)
        def _(k=k):
            t_on(k).start()
            t_sib(k, 3, cross).start()

        for d in forward_at[k]:
            w_z(0, d).wait_recv()
            w_xs(d)
        rows = chunk(k)
        acc[rows, 0:nh] += jnp.dot(xbuf[rows, block(cross)], wbuf[block(cross), 0:nh], preferred_element_type=F32)

    def finish(h, rows, kv):
        kv = kv.astype(BF16)
        key, val = kv[:, :hs], kv[:, hs:]
        k_s[h, rows, :] = key
        v_s[h, rows, :] = val
        fk = feature(key.astype(F32)).astype(BF16)
        macc[h] += lax.dot_general(fk, val, TN, preferred_element_type=F32)
        nacc[h] += jnp.sum(fk.astype(F32).reshape(rc // 8, 8, hs), axis=0)

    def cross_rows(j):
        rows = chunk(j)
        kv = acc[rows, ck]
        for i in range(1, NX):
            f = block(rem(x + i, NX))
            kv += jnp.dot(xbuf[rows, f], wbuf[f, ck], preferred_element_type=F32)
        finish(1, rows, kv)

    done(wbuf.at[pl.ds(0, wr), pl.ds(0, hs)], wyr.at[1])
    for d in ZORDER:
        w_z(1, d).start()
    w_x(1, 1, 0).start()
    w_x(1, 3, 0).start()

    done(wof.at[2, pl.ds(0, br), :], o0r.at[0])
    for d in ZORDER:
        o_z(d).start()

    def q_forward():
        done(wbuf.at[pl.ds(0, wr * (NZ - 1)), pl.ds(0, hs)], wqr.at[0])
        for d in ZORDER:
            w_x(1, 1, d).start()
            w_x(1, 3, d).start()

    last = NY - 1 - part
    for k in range(4):
        t_wait(k, 0, part)

        @pl.when(is_main)
        def _(k=k):
            t_sib(k, 0, part).start()

        if k == 3:
            done(wbuf.at[pl.ds(0, 2 * NZ * wr), pl.ds(0, 2 * hs)], wxr.at[0])
            done(wbuf.at[pl.ds(0, fs), pl.ds(0, hs)], wxr.at[2])
            done(wbuf.at[pl.ds(0, fs), pl.ds(0, hs)], wcr.at[0])

            for j in range(3):
                cross_rows(j)
            pl.when(c == 1)(q_forward)

        t_wait(k, 1, last)

        @pl.when(is_main)
        def _(k=k):
            t_sib(k, 1, last).start()

        rows = chunk(k)
        acc[rows, ck] = jnp.dot(xbuf[rows, block(x)], wbuf[block(x), ck], preferred_element_type=F32)
        add = jnp.dot(xbuf[rows, block(part)], wbuf[block(part), 0:nh], preferred_element_type=F32)
        kv = jnp.dot(xbuf[rows, block(last)], wbuf[block(last), ok], preferred_element_type=F32)
        acc[rows, oq] += add[:, oq]
        finish(0, rows, acc[rows, ok] + (kv + add[:, ok]))

    cross_rows(3)

    per_head, hw = hs // pr, hs // 2
    norms = []
    for h in range(heads):
        slot = m if h == 0 else 1 - m
        norm = jnp.sum(nacc[h], axis=0, keepdims=True)
        which = lax.broadcasted_iota(jnp.int32, (16, hw), 0)
        norms += [jnp.where(which == 2 * slot + i, norm[:, i * hw : (i + 1) * hw], 0.0) for i in range(2)]
        for p in range(per_head):
            rows = slice(p * pr, (p + 1) * pr)
            for i in range(2):
                mt[slot * per_head + p, i * pr : (i + 1) * pr, :] = macc[h, rows, i * hw : (i + 1) * hw].astype(BF16)
    for p in range(NE):
        mt[p, 2 * pr :, :] = sum(norms).astype(BF16)

    def a_copy(i):
        return remote(mt.at[rem(e + i, NE)], ga.at[e], asend.at[0], arecv.at[0], ee(i))

    def b_copy(d):
        return remote(tb, gb.at[z], bsend.at[0], brecv.at[0], zz(d))

    def c_copy(i):
        return remote(pc.at[rem(e + i, NE)], gc.at[e], csend.at[0], crecv.at[0], ee(i))

    for i in range(1, NE):
        a_copy(i).start()
    ga[e] = mt[e]
    o_pair().start()

    @pl.when(not_source)
    def _():
        o_cross().start()

    pl.when(c == 0)(q_forward)

    scale = 1.0 / hs**0.5
    lower = lax.broadcasted_iota(jnp.int32, (rc, rc), 1) <= lax.broadcasted_iota(jnp.int32, (rc, rc), 0)

    def attend(h):
        for i in range(4):
            rows = slice(i * rc, (i + 1) * rc)
            q = q_s[h, rows, :]
            diag = lax.dot_general(q, k_s[h, rows, :], NT, preferred_element_type=F32) * scale
            diag = jnp.where(lower, diag, -1e30)
            top = jnp.max(diag, axis=1, keepdims=True)
            if i:
                before = lax.dot_general(q, k_s[h, 0 : i * rc, :], NT, preferred_element_type=F32) * scale
                top = jnp.maximum(top, jnp.max(before, axis=1, keepdims=True))
                pb = jnp.exp(before - top)
            pd = jnp.exp(diag - top)
            total = jnp.sum(pd, axis=1, keepdims=True)
            got = jnp.dot(pd.astype(BF16), v_s[h, rows, :], preferred_element_type=F32)
            if i:
                total += jnp.sum(pb, axis=1, keepdims=True)
                got += jnp.dot(pb.astype(BF16), v_s[h, 0 : i * rc, :], preferred_element_type=F32)
            loc[h, rows, :] = got / total * (1.0 - shares[h])

    def own_q(j, carry):
        rows = chunk(j)
        add = jnp.dot(xbuf[rows, block(last)], wbuf[block(last), oq], preferred_element_type=F32)
        q_s[0, rows, :] = (acc[rows, oq] + add).astype(BF16)
        return carry

    lax.fori_loop(0, 4, own_q, 0)
    shares = [jax.nn.sigmoid(ls[0:1, :])]
    attend(0)

    done(ga.at[pl.ds(0, NE - 1)], arecv.at[0])
    plane = ga[0].astype(F32)
    for p in range(1, NE):
        plane += ga[p].astype(F32)
    tb[...] = plane.astype(BF16)
    for d in (4, 3, 5, 2, 6, 1, 7):

        @pl.when(z + d < NZ)
        def _(d=d):
            b_copy(d).start()

    def bulk():
        @pl.when(is_source)
        def _():
            o_cross().start()

        for i in range(1, NX):
            o_x(i).start()

    done(wof.at[2, pl.ds(0, (NZ - 1) * br), :], o1r.at[0])
    pl.when(c == 0)(bulk)

    done(wbuf.at[pl.ds(0, fs), pl.ds(0, hs)], wcr.at[1])
    done(wbuf.at[pl.ds(0, 2 * NZ * wr), pl.ds(0, hs)], wxr.at[1])
    g_copy().wait_recv()

    def cross_q(j, carry):
        rows = chunk(j)
        q_s[1, rows, :] = jnp.dot(xbuf[rows, :], wbuf[:, cq], preferred_element_type=F32).astype(BF16)
        return carry

    lax.fori_loop(0, 4, cross_q, 0)
    shares.append(jax.nn.sigmoid(lb[0:1, :]))

    attend(1)

    for n in range(1, NZ):

        @pl.when(z == n)
        def _(n=n):
            done(gb.at[pl.ds(0, n)], brecv.at[0])

    run = lax.fori_loop(0, z, lambda k, s: s + gb[k].astype(F32), jnp.zeros(tb.shape, F32))
    for p in range(NE):
        pc[p] = run.astype(BF16)
        run += ga[p].astype(F32)
    for i in range(1, NE):
        c_copy(i).start()
    gc[e] = pc[e]
    pl.when(c == 1)(bulk)

    done(gc.at[pl.ds(0, NE - 1)], crecv.at[0])
    for h in range(heads):
        slot = m if h == 0 else 1 - m
        for p in range(per_head):
            for i in range(2):
                mem[h, p * pr : (p + 1) * pr, i * hw : (i + 1) * hw] = gc[slot * per_head + p, i * pr : (i + 1) * pr, :]
        for i in range(2):
            row = 2 * pr + i
            norm = jnp.where(slot == 0, gc[0, row : row + 1, :].astype(F32), gc[0, row + 2 : row + 3, :].astype(F32))
            nrm[h, :, i * hw : (i + 1) * hw] = jnp.broadcast_to(norm, (hs, hw)).astype(BF16)

    sizes = [seg // 8] * 7 + [seg // 16] * 2
    spans = [(sum(sizes[:u]), size) for u, size in enumerate(sizes)]

    pidx = div(y * cross, 2)

    def m_ref(u, cc, pp):
        return mixs.at[pl.ds(*spans[u]), pl.ds(pl.multiple_of(cc * 4 * hs + pp * 2 * hs, hs), 2 * hs)]

    def m_pair(u, pp):
        return remote(m_ref(u, c, pp), m_ref(u, c, pp), psend.at[0], precv.at[u], {"y": part})

    def m_sib(u, pp, fin):
        return remote(m_ref(u, c, pp), m_ref(u, c, pp), fin.at[0], drecv.at[u], sibling)

    for u in range(NU):
        rows = pl.ds(*spans[u])
        for h in range(heads):
            fq = feature(q_s[h, rows, :].astype(F32)).astype(BF16)
            denom = lax.dot_general(fq, nrm[h], NT, preferred_element_type=F32)
            numer = jnp.dot(fq, mem[h], preferred_element_type=F32)
            val = shares[h] * (numer / jnp.maximum(denom, 1.0)) + loc[h, rows, :]
            at = c * 4 * hs + pidx * 2 * hs + (m if h == 0 else 1 - m) * hs
            mixs[rows, pl.ds(pl.multiple_of(at, hs), hs)] = val.astype(BF16)
        m_pair(u, pidx).start()
        m_sib(u, pidx, dsend).start()

    def o_copy(u):
        rows = pl.ds(*spans[u])
        dev = {"y": y + c * (cross - y), "c": m}
        return remote(outs.at[rows, :], out.at[rows, :], osend.at[0], orecv.at[0], dev)

    for step in range(NU + 1):
        if step < NU:
            m_pair(step, 1 - pidx).wait_recv()
            m_sib(step, 1 - pidx, fsend).start()
        if step:
            u = step - 1
            if u == 0:
                done(wof.at[2, pl.ds(0, (NX - 1) * NZ * br), :], o2r.at[0])
                done(wof.at[0], o3r.at[0])
                done(wof.at[0], o3r.at[1])
                done(wof.at[0], lsem.at[2])
            rows = pl.ds(*spans[u])
            done(mixs.at[rows, pl.ds(0, 2 * gw)], drecv.at[u])
            o = jnp.zeros((spans[u][1], fs), F32)
            for cc in range(NC):
                for pos, grp in enumerate((0, 3, 1, 2)):
                    at = cc * 4 * hs + pos * hs
                    part_w = wof[rem(grp + NY - y, NY), cc * hs : (cc + 1) * hs, :]
                    o += jnp.dot(mixs[rows, at : at + hs], part_w, preferred_element_type=F32)
            outs[rows, :] = o.astype(BF16)

            @pl.when(at_home)
            def _(rows=rows):
                fetch(outs.at[rows, :], out.at[rows, :], 3)

            @pl.when(jnp.logical_not(at_home))
            def _(u=u):
                o_copy(u).start()

    @pl.when(at_home)
    def _():
        done(outs, lsem.at[3])

    @pl.when(jnp.logical_not(at_home))
    def _():
        done(outs, osend.at[0])

    @pl.when(jnp.logical_not(at_home))
    def _():
        done(outs, orecv.at[0])

    done(outs, psend.at[0])
    done(outs, dsend.at[0])
    done(outs, fsend.at[0])

    @pl.when(is_source)
    def _():
        done(xbuf.at[:, pl.ds(0, 2 * fs)], tsend.at[0])

    @pl.when(is_main)
    def _():
        done(xbuf, tsend.at[1])

    @pl.when(not_source)
    def _():
        done(xbuf.at[:, pl.ds(0, fs)], tsend.at[0])
        done(wbuf.at[pl.ds(0, fs), pl.ds(0, 2 * gw)], wcs.at[0])

    done(wbuf.at[pl.ds(0, wr), pl.ds(0, nh)], wys.at[0])
    done(wbuf.at[pl.ds(0, (NZ - 1) * wr), pl.ds(0, nh)], wzs.at[0])
    done(wbuf.at[pl.ds(0, 2 * NZ * wr), pl.ds(0, 2 * hs)], wxs.at[0])
    done(wbuf.at[pl.ds(0, 2 * NZ * wr), pl.ds(0, hs)], wxs.at[1])
    done(wbuf.at[pl.ds(0, fs), pl.ds(0, hs)], wxs.at[2])
    g_copy().wait_send()

    done(wof.at[2, pl.ds(0, br), :], o0s.at[0])
    done(wof.at[2, pl.ds(0, (NZ - 1) * br), :], o1s.at[0])
    done(wof.at[2, pl.ds(0, (NX - 1) * NZ * br), :], o2s.at[0])
    done(wof.at[pl.ds(0, 2)], o3s.at[0])
    done(ga.at[pl.ds(0, NE - 1)], asend.at[0])
    done(gc.at[pl.ds(0, NE - 1)], csend.at[0])
    for n in range(1, NZ):

        @pl.when(z == NZ - 1 - n)
        def _(n=n):
            done(gb.at[pl.ds(0, n)], bsend.at[0])


def on_device(tokens, w_query, w_key, w_value, w_out, mix_logit):
    seg, fs = tokens.shape
    heads = mix_logit.shape[0]
    gw = w_query.shape[1]
    hs = gw // heads
    pr = heads * hs // NE
    hbm = pl.BlockSpec(memory_space=pl.ANY)
    dma = pltpu.SemaphoreType.DMA
    return pl.pallas_call(
        kernel,
        out_shape=jax.ShapeDtypeStruct((seg, fs), BF16),
        in_specs=[hbm] * 5 + [pl.BlockSpec(memory_space=pltpu.SMEM)],
        out_specs=hbm,
        scratch_shapes=[
            pltpu.VMEM((seg, NY * fs), BF16),
            pltpu.VMEM((NY * fs, 3 * gw), BF16),
            pltpu.VMEM((seg, 3 * gw), F32),
            pltpu.VMEM((heads, seg, hs), BF16),
            pltpu.VMEM((heads, seg, hs), BF16),
            pltpu.VMEM((heads, seg, hs), BF16),
            pltpu.VMEM((heads, seg, hs), F32),
            pltpu.VMEM((NY, gw, fs), BF16),
            pltpu.VMEM((heads, hs, hs), F32),
            pltpu.VMEM((heads, 8, hs), F32),
            pltpu.VMEM((NE, 2 * pr + 16, hs // 2), BF16),
            pltpu.VMEM((NE, 2 * pr + 16, hs // 2), BF16),
            pltpu.VMEM((2 * pr + 16, hs // 2), BF16),
            pltpu.VMEM((NZ, 2 * pr + 16, hs // 2), BF16),
            pltpu.VMEM((NE, 2 * pr + 16, hs // 2), BF16),
            pltpu.VMEM((NE, 2 * pr + 16, hs // 2), BF16),
            pltpu.VMEM((heads, hs, hs), BF16),
            pltpu.VMEM((heads, hs, hs), BF16),
            pltpu.VMEM((seg, NY * gw), BF16),
            pltpu.VMEM((seg, fs), BF16),
            pltpu.VMEM((8, hs), F32),
            pltpu.VMEM((8, hs), F32),
            dma((4,)),
            dma((2,)), dma((4, 4)),
            dma((1,)), dma((2,)),
            dma((1,)), dma((NZ,)), dma((1,)),
            dma((3,)), dma((3,)),
            dma((1,)), dma((2,)),
            dma((1,)), dma((1,)),
            dma((1,)), dma((1,)),
            dma((1,)), dma((1,)),
            dma((1,)), dma((2,)),
            dma((1,)), dma((1,)),
            dma((1,)), dma((1,)),
            dma((1,)), dma((1,)),
            dma((1,)), dma((1,)),
            dma((1,)), dma((NU,)),
            dma((1,)), dma((NU,)),
            dma((1,)),
            dma((1,)), dma((1,)),
        ],
        compiler_params=pltpu.CompilerParams(
            collective_id=0, has_side_effects=True, vmem_limit_bytes=52 * 2**20
        ),
    )(tokens, w_query, w_key, w_value, w_out, mix_logit)


def solution(mesh):
    torus = Mesh(mesh.devices.reshape(NZ, NX, NC, NY), ("z", "x", "c", "y"))
    return jax.shard_map(
        on_device,
        mesh=torus,
        in_specs=(P(SEQ, "y"), P(None, "y"), P(None, "y"), P(None, "y"), P("y", None), P("y")),
        out_specs=P(SEQ, "y"),
        check_vma=False,
    )
```

```python
import functools

import jax
import jax.numpy as jnp
from jax import lax
from jax.experimental import pallas as pl
from jax.experimental.pallas import tpu as pltpu
from jax.sharding import Mesh
from jax.sharding import PartitionSpec as P

SEQ = ("z", "x", "c")
MESH = pl.DeviceIdType.MESH
F32, BF16 = jnp.float32, jnp.bfloat16
NZ, NX, NC, NY = 8, 4, 2, 4
NE = NX * NC
NU = 9
ZORDER = (1, 7, 2, 6, 3, 5, 4)
NT = (((1,), (1,)), ((), ()))
TN = (((0,), (0,)), ((), ()))


def feature(values):
    return jnp.where(values > 0, values + 1.0, jnp.exp(values))


def kernel(
    tok, wq, wk, wv, wo, logit, out,
    xbuf, wbuf, acc, q_s, k_s, v_s, loc, wof, macc, nacc, mt, ga, tb, gb, pc, gc, mem, nrm, mixs, outs, ls, lb,
    lsem, tsend, trecv, wys, wyr, wzs, wzr, wqr, wxs, wxr, wcs, wcr, o0s, o0r, o1s, o1r, o2s, o2r, o3s, o3r, gsend, grecv,
    asend, arecv, bsend, brecv, csend, crecv, psend, precv, dsend, drecv, fsend, osend, orecv,
):
    z, x, c, y = (lax.axis_index(a) for a in ("z", "x", "c", "y"))
    rem, div = lax.rem, lax.div
    m = div(y, 2)
    part = y + 1 - 2 * rem(y, 2)
    cross = NY - 1 - y
    g = y + c * (cross - y)
    gp = g + 1 - 2 * rem(g, 2)
    e = x * NC + m
    seg, fs = tok.shape
    heads, _, hs = q_s.shape
    rc = seg // 4
    gw = heads * hs
    pr = heads * hs // NE
    br = gw // (NZ * NX)
    wr = NY * fs // (NZ * NX)
    is_source, not_source = c == m, c != m
    is_main = c == 1
    at_home = c + m == 0

    def yy(r):
        return {"y": rem(y + r, NY)}

    def zz(d):
        return {"z": rem(z + d, NZ)}

    def xx(i):
        return {"x": rem(x + i, NX)}

    def ee(i):
        o = rem(e + i, NE)
        par = rem(o, NC)
        diff = par + m - 2 * par * m
        return {"x": div(o, NC), "y": y + diff * (cross - y)}

    sibling = {"c": 1 - c}

    def remote(src, dst, ssem, rsem, dev):
        return pltpu.make_async_remote_copy(
            src_ref=src, dst_ref=dst, send_sem=ssem, recv_sem=rsem, device_id=dev, device_id_type=MESH
        )

    def fetch(src, dst, k):
        pltpu.make_async_copy(src, dst, lsem.at[k]).start()

    def done(ref, sem):
        pltpu.make_async_copy(ref, ref, sem).wait()

    def chunk(j):
        return pl.ds(pl.multiple_of(j * rc, rc), rc)

    pieces = [(0, rc), (rc, rc), (2 * rc, rc), (3 * rc, rc // 2), (3 * rc + rc // 2, rc // 2)]
    nk = len(pieces)

    def part_rows(k):
        return pl.ds(*pieces[k])

    def block(f):
        return pl.ds(pl.multiple_of(f * fs, fs), fs)

    def group(f):
        return pl.ds(pl.multiple_of(f * gw, gw), gw)

    barrier = pltpu.get_barrier_semaphore()
    peers = [zz(d) for d in range(1, NZ)] + [yy(r) for r in range(1, NY)] + [xx(i) for i in range(1, NX)]
    peers += [{"x": rem(x + i, NX), "y": cross} for i in range(1, NX)] + [sibling, {"y": cross, "c": 1 - c}, {"y": part, "c": 1 - c}]
    for dev in peers:
        pl.semaphore_signal(barrier, inc=1, device_id=dev, device_id_type=MESH)

    ls[...] = jnp.full(ls.shape, logit[c], F32)

    weights = (wk, wv, wq)
    nh = 3 * hs
    ok, oq = slice(0, 2 * hs), slice(2 * hs, nh)
    ck, cq = slice(nh, nh + 2 * hs), slice(nh + 2 * hs, 2 * nh)

    def head(ct):
        return pl.ds(pl.multiple_of(ct * hs, hs), hs)

    @pl.when(is_source)
    def _():
        fetch(tok, xbuf.at[:, block(y)], 0)

    for i, w in enumerate(weights):
        fetch(w.at[:, head(c)], wbuf.at[:, pl.ds(i * hs, hs)], 1)

    fetch(wo.at[:, group(g)], wof.at[0], 2)

    pl.semaphore_wait(barrier, len(peers))

    def t_pair(k):
        return remote(
            tok.at[part_rows(k), :], xbuf.at[part_rows(k), block(y)], tsend.at[0], trecv.at[0, k], {"y": part, "c": 1}
        )

    def t_cross(k):
        return remote(
            tok.at[part_rows(k), :], xbuf.at[part_rows(k), block(y)], tsend.at[0], trecv.at[3, k], {"y": cross, "c": 1}
        )

    def t_on(k):
        ref = xbuf.at[part_rows(k), block(cross)]
        return remote(ref, ref, tsend.at[1], trecv.at[1, k], {"y": part})

    def t_sib(k, kind, f):
        ref = xbuf.at[part_rows(k), block(f)]
        return remote(ref, ref, tsend.at[1], trecv.at[kind, k], sibling)

    def t_own():
        return remote(tok, xbuf.at[:, block(y)], tsend.at[0], trecv.at[2, 0], sibling)

    def t_wait(k, kind, f):
        t_sib(k, kind, f).wait_recv()

    def w_rows(xp, zp):
        return pl.ds(pl.multiple_of((xp * NZ + zp) * wr, wr), wr)

    far_block = rem(x + 2, NX)
    w_cols = (pl.ds(nh, 2 * hs), pl.ds(nh + 2 * hs, hs), pl.ds(nh + hs, hs))

    def w_piece(i):
        return remote(
            weights[i].at[w_rows(x, z), head(c)], wbuf.at[w_rows(x, z), pl.ds(nh + i * hs, hs)],
            wys.at[0], wyr.at[i // 2], {"y": cross},
        )

    def w_z(kind, d):
        ref = wbuf.at[w_rows(x, z), w_cols[kind]]
        return remote(ref, ref, wzs.at[0], wqr.at[0] if kind else wzr.at[d], zz(d))

    def w_x(kind, i, d):
        ref = wbuf.at[w_rows(x, rem(z + NZ - d, NZ)), w_cols[kind]]
        return remote(ref, ref, wxs.at[kind], wxr.at[kind], xx(i))

    def w_xs(d):
        w_x(0, 1, d).start()
        w_x(0, 3, d).start()

        @pl.when(c == 0)
        def _():
            w_x(2, 2, d).start()

    def w_cross(i, ct):
        return remote(
            weights[i].at[block(far_block), head(ct)], wbuf.at[block(far_block), pl.ds(nh + i * hs, hs)],
            wcs.at[0], wcr.at[i // 2], {"y": cross, "c": ct},
        )

    def o_rows(xp, zp):
        return pl.ds(pl.multiple_of((xp * NZ + zp) * br, br), br)

    def o_y():
        return remote(
            wo.at[o_rows(x, z), group(NY - 1 - gp)], wof.at[2, o_rows(x, z), :], o0s.at[0], o0r.at[0], yy(2)
        )

    def o_z(d):
        ref = wof.at[2, o_rows(x, z), :]
        return remote(ref, ref, o1s.at[0], o1r.at[0], zz(d))

    def o_x(i):
        ref = wof.at[2, pl.ds(pl.multiple_of(x * NZ * br, NZ * br), NZ * br), :]
        return remote(ref, ref, o2s.at[0], o2r.at[0], xx(i))

    def o_pair():
        return remote(
            wo.at[:, group(gp)], wof.at[3 - 2 * rem(y, 2)], o3s.at[0], o3r.at[0], {"y": part}
        )

    def o_cross():
        return remote(
            wo.at[:, group(NY - 1 - g)], wof.at[1 + 2 * rem(y, 2)], o3s.at[0], o3r.at[1], {"y": cross}
        )

    def g_copy():
        return remote(ls, lb, gsend.at[0], grecv.at[0], {"y": cross})

    for i in range(2):
        w_piece(i).start()
    o_y().start()

    @pl.when(is_source)
    def _():
        for k in range(nk):
            t_pair(k).start()
        t_own().start()

    @pl.when(not_source)
    def _():
        for k in range(nk):
            t_cross(k).start()

    w_piece(2).start()
    g_copy().start()

    @pl.when(not_source)
    def _():
        for i, ct in ((0, 1), (1, 1), (0, 0), (2, 1), (2, 0)):
            w_cross(i, ct).start()

    macc[...] = jnp.zeros_like(macc)
    nacc[...] = jnp.zeros_like(nacc)

    @pl.when(is_source)
    def _():
        done(xbuf.at[:, block(y)], lsem.at[0])

    @pl.when(not_source)
    def _():
        t_own().wait_recv()

    done(wbuf.at[:, pl.ds(0, nh)], lsem.at[1])

    def own_dot(j, carry):
        acc[chunk(j), 0:nh] = jnp.dot(
            xbuf[chunk(j), block(y)], wbuf[block(y), 0:nh], preferred_element_type=F32
        )
        return carry

    lax.fori_loop(0, 2, own_dot, 0)
    done(wbuf.at[pl.ds(0, wr), pl.ds(0, 2 * hs)], wyr.at[0])
    for d in ZORDER:
        w_z(0, d).start()
    w_xs(0)
    lax.fori_loop(2, 4, own_dot, 0)

    forward_at = {0: (1, 7), 1: (2, 6), 2: (3, 5), 3: (4,), 4: ()}
    for k in range(nk):
        t_wait(k, 3, cross)

        @pl.when(is_main)
        def _(k=k):
            t_on(k).start()
            t_sib(k, 3, cross).start()

        for d in forward_at[k]:
            w_z(0, d).wait_recv()
            w_xs(d)
        rows = part_rows(k)
        acc[rows, 0:nh] += jnp.dot(xbuf[rows, block(cross)], wbuf[block(cross), 0:nh], preferred_element_type=F32)

    def finish(h, rows, kv):
        kv = kv.astype(BF16)
        key, val = kv[:, :hs], kv[:, hs:]
        k_s[h, rows, :] = key
        v_s[h, rows, :] = val
        fk = feature(key.astype(F32)).astype(BF16)
        macc[h] += lax.dot_general(fk, val, TN, preferred_element_type=F32)
        nacc[h] += jnp.sum(fk.astype(F32).reshape(-1, 8, hs), axis=0)

    def cross_rows(k):
        rows = part_rows(k)
        kv = acc[rows, ck]
        for i in range(1, NX):
            f = block(rem(x + i, NX))
            kv += jnp.dot(xbuf[rows, f], wbuf[f, ck], preferred_element_type=F32)
        finish(1, rows, kv)

    done(wbuf.at[pl.ds(0, wr), pl.ds(0, hs)], wyr.at[1])
    for d in ZORDER:
        w_z(1, d).start()
    w_x(1, 1, 0).start()
    w_x(1, 3, 0).start()

    done(wof.at[2, pl.ds(0, br), :], o0r.at[0])
    for d in ZORDER:
        o_z(d).start()

    def q_forward():
        done(wbuf.at[pl.ds(0, wr * (NZ - 1)), pl.ds(0, hs)], wqr.at[0])
        for d in ZORDER:
            w_x(1, 1, d).start()
            w_x(1, 3, d).start()

    last = NY - 1 - part
    for k in range(nk):
        if k == 2:

            @pl.when(c == 1)
            def _():
                done(wbuf.at[pl.ds(0, 2 * NZ * wr), pl.ds(0, 2 * hs)], wxr.at[0])
                done(wbuf.at[pl.ds(0, fs), pl.ds(0, 2 * hs)], wcr.at[0])
                cross_rows(0)
                cross_rows(1)

        if k == 3:

            @pl.when(c == 0)
            def _():
                done(wbuf.at[pl.ds(0, 2 * NZ * wr), pl.ds(0, 2 * hs)], wxr.at[0])
                done(wbuf.at[pl.ds(0, fs), pl.ds(0, hs)], wxr.at[2])
                done(wbuf.at[pl.ds(0, fs), pl.ds(0, hs)], wcr.at[0])
                cross_rows(0)
                cross_rows(1)

            cross_rows(2)
            pl.when(c == 1)(q_forward)

        t_wait(k, 0, part)

        @pl.when(is_main)
        def _(k=k):
            t_sib(k, 0, part).start()

        t_wait(k, 1, last)

        @pl.when(is_main)
        def _(k=k):
            t_sib(k, 1, last).start()

        rows = part_rows(k)
        acc[rows, ck] = jnp.dot(xbuf[rows, block(x)], wbuf[block(x), ck], preferred_element_type=F32)
        add = jnp.dot(xbuf[rows, block(part)], wbuf[block(part), 0:nh], preferred_element_type=F32)
        kv = jnp.dot(xbuf[rows, block(last)], wbuf[block(last), ok], preferred_element_type=F32)
        acc[rows, oq] += add[:, oq]
        finish(0, rows, acc[rows, ok] + (kv + add[:, ok]))
        if k >= 3:
            cross_rows(k)

    per_head, hw = hs // pr, hs // 2
    norms = []
    for h in range(heads):
        slot = m if h == 0 else 1 - m
        norm = jnp.sum(nacc[h], axis=0, keepdims=True)
        which = lax.broadcasted_iota(jnp.int32, (16, hw), 0)
        norms += [jnp.where(which == 2 * slot + i, norm[:, i * hw : (i + 1) * hw], 0.0) for i in range(2)]
        for p in range(per_head):
            rows = slice(p * pr, (p + 1) * pr)
            for i in range(2):
                mt[slot * per_head + p, i * pr : (i + 1) * pr, :] = macc[h, rows, i * hw : (i + 1) * hw].astype(BF16)
    for p in range(NE):
        mt[p, 2 * pr :, :] = sum(norms).astype(BF16)

    def a_copy(i):
        return remote(mt.at[rem(e + i, NE)], ga.at[e], asend.at[0], arecv.at[0], ee(i))

    def b_copy(d):
        return remote(tb, gb.at[z], bsend.at[0], brecv.at[0], zz(d))

    def c_copy(i):
        return remote(pc.at[rem(e + i, NE)], gc.at[e], csend.at[0], crecv.at[0], ee(i))

    for i in range(1, NE):
        a_copy(i).start()
    ga[e] = mt[e]
    o_pair().start()

    @pl.when(not_source)
    def _():
        o_cross().start()

    pl.when(c == 0)(q_forward)

    scale = 1.0 / hs**0.5
    lower = lax.broadcasted_iota(jnp.int32, (rc, rc), 1) <= lax.broadcasted_iota(jnp.int32, (rc, rc), 0)

    def attend(h):
        for i in range(4):
            rows = slice(i * rc, (i + 1) * rc)
            q = q_s[h, rows, :]
            diag = lax.dot_general(q, k_s[h, rows, :], NT, preferred_element_type=F32) * scale
            diag = jnp.where(lower, diag, -1e30)
            top = jnp.max(diag, axis=1, keepdims=True)
            if i:
                before = lax.dot_general(q, k_s[h, 0 : i * rc, :], NT, preferred_element_type=F32) * scale
                top = jnp.maximum(top, jnp.max(before, axis=1, keepdims=True))
                pb = jnp.exp(before - top)
            pd = jnp.exp(diag - top)
            total = jnp.sum(pd, axis=1, keepdims=True)
            got = jnp.dot(pd.astype(BF16), v_s[h, rows, :], preferred_element_type=F32)
            if i:
                total += jnp.sum(pb, axis=1, keepdims=True)
                got += jnp.dot(pb.astype(BF16), v_s[h, 0 : i * rc, :], preferred_element_type=F32)
            loc[h, rows, :] = got / total * (1.0 - shares[h])

    def own_q(j, carry):
        rows = chunk(j)
        add = jnp.dot(xbuf[rows, block(last)], wbuf[block(last), oq], preferred_element_type=F32)
        q_s[0, rows, :] = (acc[rows, oq] + add).astype(BF16)
        return carry

    lax.fori_loop(0, 4, own_q, 0)
    shares = [jax.nn.sigmoid(ls[0:1, :])]
    attend(0)

    done(ga.at[pl.ds(0, NE - 1)], arecv.at[0])
    plane = ga[0].astype(F32)
    for p in range(1, NE):
        plane += ga[p].astype(F32)
    tb[...] = plane.astype(BF16)
    for d in (4, 3, 5, 2, 6, 1, 7):

        @pl.when(z + d < NZ)
        def _(d=d):
            b_copy(d).start()

    def bulk():
        @pl.when(is_source)
        def _():
            o_cross().start()

        for i in range(1, NX):
            o_x(i).start()

    done(wof.at[2, pl.ds(0, (NZ - 1) * br), :], o1r.at[0])

    done(wbuf.at[pl.ds(0, fs), pl.ds(0, hs)], wcr.at[1])
    done(wbuf.at[pl.ds(0, 2 * NZ * wr), pl.ds(0, hs)], wxr.at[1])
    g_copy().wait_recv()

    def cross_q(j, carry):
        rows = chunk(j)
        q_s[1, rows, :] = jnp.dot(xbuf[rows, :], wbuf[:, cq], preferred_element_type=F32).astype(BF16)
        return carry

    lax.fori_loop(0, 4, cross_q, 0)
    shares.append(jax.nn.sigmoid(lb[0:1, :]))

    attend(1)

    for n in range(1, NZ):

        @pl.when(z == n)
        def _(n=n):
            done(gb.at[pl.ds(0, n)], brecv.at[0])

    run = lax.fori_loop(0, z, lambda k, s: s + gb[k].astype(F32), jnp.zeros(tb.shape, F32))
    for p in range(NE):
        pc[p] = run.astype(BF16)
        run += ga[p].astype(F32)
    for i in range(1, NE):
        c_copy(i).start()
    gc[e] = pc[e]
    pl.when(c == 0)(bulk)

    done(gc.at[pl.ds(0, NE - 1)], crecv.at[0])
    pl.when(c == 1)(bulk)
    for h in range(heads):
        slot = m if h == 0 else 1 - m
        for p in range(per_head):
            for i in range(2):
                mem[h, p * pr : (p + 1) * pr, i * hw : (i + 1) * hw] = gc[slot * per_head + p, i * pr : (i + 1) * pr, :]
        for i in range(2):
            row = 2 * pr + i
            norm = jnp.where(slot == 0, gc[0, row : row + 1, :].astype(F32), gc[0, row + 2 : row + 3, :].astype(F32))
            nrm[h, :, i * hw : (i + 1) * hw] = jnp.broadcast_to(norm, (hs, hw)).astype(BF16)

    sizes = [seg // 8] * 7 + [seg // 16] * 2
    spans = [(sum(sizes[:u]), size) for u, size in enumerate(sizes)]

    pidx = div(y * cross, 2)

    def m_ref(u, cc, pp):
        return mixs.at[pl.ds(*spans[u]), pl.ds(pl.multiple_of(cc * 4 * hs + pp * 2 * hs, hs), 2 * hs)]

    def m_pair(u, pp):
        return remote(m_ref(u, c, pp), m_ref(u, c, pp), psend.at[0], precv.at[u], {"y": part})

    def m_sib(u, pp, fin):
        return remote(m_ref(u, c, pp), m_ref(u, c, pp), fin.at[0], drecv.at[u], sibling)

    for u in range(NU):
        rows = pl.ds(*spans[u])
        for h in range(heads):
            fq = feature(q_s[h, rows, :].astype(F32)).astype(BF16)
            denom = lax.dot_general(fq, nrm[h], NT, preferred_element_type=F32)
            numer = jnp.dot(fq, mem[h], preferred_element_type=F32)
            val = shares[h] * (numer / jnp.maximum(denom, 1.0)) + loc[h, rows, :]
            at = c * 4 * hs + pidx * 2 * hs + (m if h == 0 else 1 - m) * hs
            mixs[rows, pl.ds(pl.multiple_of(at, hs), hs)] = val.astype(BF16)
        m_pair(u, pidx).start()
        m_sib(u, pidx, dsend).start()

    def o_copy(u):
        rows = pl.ds(*spans[u])
        dev = {"y": y + c * (cross - y), "c": m}
        return remote(outs.at[rows, :], out.at[rows, :], osend.at[0], orecv.at[0], dev)

    for step in range(NU + 1):
        if step < NU:
            m_pair(step, 1 - pidx).wait_recv()
            m_sib(step, 1 - pidx, fsend).start()
        if step:
            u = step - 1
            if u == 0:
                done(wof.at[2, pl.ds(0, (NX - 1) * NZ * br), :], o2r.at[0])
                done(wof.at[0], o3r.at[0])
                done(wof.at[0], o3r.at[1])
                done(wof.at[0], lsem.at[2])
            rows = pl.ds(*spans[u])
            done(mixs.at[rows, pl.ds(0, 2 * gw)], drecv.at[u])
            o = jnp.zeros((spans[u][1], fs), F32)
            for cc in range(NC):
                for pos, grp in enumerate((0, 3, 1, 2)):
                    at = cc * 4 * hs + pos * hs
                    part_w = wof[rem(grp + NY - y, NY), cc * hs : (cc + 1) * hs, :]
                    o += jnp.dot(mixs[rows, at : at + hs], part_w, preferred_element_type=F32)
            outs[rows, :] = o.astype(BF16)

            @pl.when(at_home)
            def _(rows=rows):
                fetch(outs.at[rows, :], out.at[rows, :], 3)

            @pl.when(jnp.logical_not(at_home))
            def _(u=u):
                o_copy(u).start()

    @pl.when(at_home)
    def _():
        done(outs, lsem.at[3])

    @pl.when(jnp.logical_not(at_home))
    def _():
        done(outs, osend.at[0])

    @pl.when(jnp.logical_not(at_home))
    def _():
        done(outs, orecv.at[0])

    done(outs, psend.at[0])
    done(outs, dsend.at[0])
    done(outs, fsend.at[0])

    @pl.when(is_source)
    def _():
        done(xbuf.at[:, pl.ds(0, 2 * fs)], tsend.at[0])

    @pl.when(is_main)
    def _():
        done(xbuf, tsend.at[1])

    @pl.when(not_source)
    def _():
        done(xbuf.at[:, pl.ds(0, fs)], tsend.at[0])
        done(wbuf.at[pl.ds(0, fs), pl.ds(0, 5 * hs)], wcs.at[0])

    done(wbuf.at[pl.ds(0, wr), pl.ds(0, nh)], wys.at[0])
    done(wbuf.at[pl.ds(0, (NZ - 1) * wr), pl.ds(0, nh)], wzs.at[0])
    done(wbuf.at[pl.ds(0, 2 * NZ * wr), pl.ds(0, 2 * hs)], wxs.at[0])
    done(wbuf.at[pl.ds(0, 2 * NZ * wr), pl.ds(0, hs)], wxs.at[1])

    @pl.when(c == 0)
    def _():
        done(wbuf.at[pl.ds(0, fs), pl.ds(0, hs)], wxs.at[2])

    g_copy().wait_send()

    done(wof.at[2, pl.ds(0, br), :], o0s.at[0])
    done(wof.at[2, pl.ds(0, (NZ - 1) * br), :], o1s.at[0])
    done(wof.at[2, pl.ds(0, (NX - 1) * NZ * br), :], o2s.at[0])
    done(wof.at[pl.ds(0, 2)], o3s.at[0])
    done(ga.at[pl.ds(0, NE - 1)], asend.at[0])
    done(gc.at[pl.ds(0, NE - 1)], csend.at[0])
    for n in range(1, NZ):

        @pl.when(z == NZ - 1 - n)
        def _(n=n):
            done(gb.at[pl.ds(0, n)], bsend.at[0])


def on_device(tokens, w_query, w_key, w_value, w_out, mix_logit):
    seg, fs = tokens.shape
    heads = mix_logit.shape[0]
    gw = w_query.shape[1]
    hs = gw // heads
    pr = heads * hs // NE
    hbm = pl.BlockSpec(memory_space=pl.ANY)
    dma = pltpu.SemaphoreType.DMA
    return pl.pallas_call(
        kernel,
        out_shape=jax.ShapeDtypeStruct((seg, fs), BF16),
        in_specs=[hbm] * 5 + [pl.BlockSpec(memory_space=pltpu.SMEM)],
        out_specs=hbm,
        scratch_shapes=[
            pltpu.VMEM((seg, NY * fs), BF16),
            pltpu.VMEM((NY * fs, 3 * gw), BF16),
            pltpu.VMEM((seg, 3 * gw), F32),
            pltpu.VMEM((heads, seg, hs), BF16),
            pltpu.VMEM((heads, seg, hs), BF16),
            pltpu.VMEM((heads, seg, hs), BF16),
            pltpu.VMEM((heads, seg, hs), F32),
            pltpu.VMEM((NY, gw, fs), BF16),
            pltpu.VMEM((heads, hs, hs), F32),
            pltpu.VMEM((heads, 8, hs), F32),
            pltpu.VMEM((NE, 2 * pr + 16, hs // 2), BF16),
            pltpu.VMEM((NE, 2 * pr + 16, hs // 2), BF16),
            pltpu.VMEM((2 * pr + 16, hs // 2), BF16),
            pltpu.VMEM((NZ, 2 * pr + 16, hs // 2), BF16),
            pltpu.VMEM((NE, 2 * pr + 16, hs // 2), BF16),
            pltpu.VMEM((NE, 2 * pr + 16, hs // 2), BF16),
            pltpu.VMEM((heads, hs, hs), BF16),
            pltpu.VMEM((heads, hs, hs), BF16),
            pltpu.VMEM((seg, NY * gw), BF16),
            pltpu.VMEM((seg, fs), BF16),
            pltpu.VMEM((8, hs), F32),
            pltpu.VMEM((8, hs), F32),
            dma((4,)),
            dma((2,)), dma((4, 5)),
            dma((1,)), dma((2,)),
            dma((1,)), dma((NZ,)), dma((1,)),
            dma((3,)), dma((3,)),
            dma((1,)), dma((2,)),
            dma((1,)), dma((1,)),
            dma((1,)), dma((1,)),
            dma((1,)), dma((1,)),
            dma((1,)), dma((2,)),
            dma((1,)), dma((1,)),
            dma((1,)), dma((1,)),
            dma((1,)), dma((1,)),
            dma((1,)), dma((1,)),
            dma((1,)), dma((NU,)),
            dma((1,)), dma((NU,)),
            dma((1,)),
            dma((1,)), dma((1,)),
        ],
        compiler_params=pltpu.CompilerParams(
            collective_id=0, has_side_effects=True, vmem_limit_bytes=52 * 2**20
        ),
    )(tokens, w_query, w_key, w_value, w_out, mix_logit)


def solution(mesh):
    torus = Mesh(mesh.devices.reshape(NZ, NX, NC, NY), ("z", "x", "c", "y"))
    return jax.shard_map(
        on_device,
        mesh=torus,
        in_specs=(P(SEQ, "y"), P(None, "y"), P(None, "y"), P(None, "y"), P("y", None), P("y")),
        out_specs=P(SEQ, "y"),
        check_vma=False,
    )
```

```python
import functools

import jax
import jax.numpy as jnp
from jax import lax
from jax.experimental import pallas as pl
from jax.experimental.pallas import tpu as pltpu
from jax.sharding import Mesh
from jax.sharding import PartitionSpec as P

SEQ = ("z", "x", "c")
MESH = pl.DeviceIdType.MESH
F32, BF16 = jnp.float32, jnp.bfloat16
NZ, NX, NC, NY = 8, 4, 2, 4
NE = NX * NC
NU = 9
ZORDER = (1, 7, 2, 6, 3, 5, 4)
NT = (((1,), (1,)), ((), ()))
TN = (((0,), (0,)), ((), ()))


def feature(values):
    return jnp.where(values > 0, values + 1.0, jnp.exp(values))


def kernel(
    tok, wq, wk, wv, wo, logit, out,
    xbuf, wbuf, acc, q_s, k_s, v_s, loc, wof, macc, nacc, mt, ga, tb, gb, pc, gc, mem, nrm, mixs, outs, ls, lb,
    lsem, tsend, trecv, wys, wyr, wzs, wzr, wqr, wxs, wxr, wcs, wcr, o0s, o0r, o1s, o1r, o2s, o2r, o3s, o3r, gsend, grecv,
    asend, arecv, bsend, brecv, csend, crecv, psend, precv, dsend, drecv, fsend, osend, orecv,
):
    z, x, c, y = (lax.axis_index(a) for a in ("z", "x", "c", "y"))
    rem, div = lax.rem, lax.div
    m = div(y, 2)
    part = y + 1 - 2 * rem(y, 2)
    cross = NY - 1 - y
    g = y + c * (cross - y)
    gp = g + 1 - 2 * rem(g, 2)
    e = x * NC + m
    seg, fs = tok.shape
    heads, _, hs = q_s.shape
    rc = seg // 4
    gw = heads * hs
    pr = heads * hs // NE
    br = gw // (NZ * NX)
    wr = NY * fs // (NZ * NX)
    is_source, not_source = c == m, c != m
    is_main = c == 1
    at_home = c + m == 0

    def yy(r):
        return {"y": rem(y + r, NY)}

    def zz(d):
        return {"z": rem(z + d, NZ)}

    def xx(i):
        return {"x": rem(x + i, NX)}

    def ee(i):
        o = rem(e + i, NE)
        par = rem(o, NC)
        diff = par + m - 2 * par * m
        return {"x": div(o, NC), "y": y + diff * (cross - y)}

    sibling = {"c": 1 - c}

    def remote(src, dst, ssem, rsem, dev):
        return pltpu.make_async_remote_copy(
            src_ref=src, dst_ref=dst, send_sem=ssem, recv_sem=rsem, device_id=dev, device_id_type=MESH
        )

    def fetch(src, dst, k):
        pltpu.make_async_copy(src, dst, lsem.at[k]).start()

    def done(ref, sem):
        pltpu.make_async_copy(ref, ref, sem).wait()

    def chunk(j):
        return pl.ds(pl.multiple_of(j * rc, rc), rc)

    pieces = [(0, rc), (rc, rc), (2 * rc, rc), (3 * rc, rc // 2), (3 * rc + rc // 2, rc // 2)]
    nk = len(pieces)

    def part_rows(k):
        return pl.ds(*pieces[k])

    def block(f):
        return pl.ds(pl.multiple_of(f * fs, fs), fs)

    def group(f):
        return pl.ds(pl.multiple_of(f * gw, gw), gw)

    barrier = pltpu.get_barrier_semaphore()
    peers = [zz(d) for d in range(1, NZ)] + [yy(r) for r in range(1, NY)] + [xx(i) for i in range(1, NX)]
    peers += [{"x": rem(x + i, NX), "y": cross} for i in range(1, NX)] + [sibling, {"y": cross, "c": 1 - c}, {"y": part, "c": 1 - c}]
    for dev in peers:
        pl.semaphore_signal(barrier, inc=1, device_id=dev, device_id_type=MESH)

    ls[...] = jnp.full(ls.shape, logit[c], F32)

    weights = (wk, wv, wq)
    nh = 3 * hs
    ok, oq = slice(0, 2 * hs), slice(2 * hs, nh)
    ck, cq = slice(nh, nh + 2 * hs), slice(nh + 2 * hs, 2 * nh)

    def head(ct):
        return pl.ds(pl.multiple_of(ct * hs, hs), hs)

    @pl.when(is_source)
    def _():
        fetch(tok, xbuf.at[:, block(y)], 0)

    for i, w in enumerate(weights):
        fetch(w.at[:, head(c)], wbuf.at[:, pl.ds(i * hs, hs)], 1)

    fetch(wo.at[:, group(g)], wof.at[0], 2)

    pl.semaphore_wait(barrier, len(peers))

    def t_pair(k):
        return remote(
            tok.at[part_rows(k), :], xbuf.at[part_rows(k), block(y)], tsend.at[0], trecv.at[0, k], {"y": part, "c": 1}
        )

    def t_cross(k):
        return remote(
            tok.at[part_rows(k), :], xbuf.at[part_rows(k), block(y)], tsend.at[0], trecv.at[3, k], {"y": cross, "c": 1}
        )

    def t_on(k):
        ref = xbuf.at[part_rows(k), block(cross)]
        return remote(ref, ref, tsend.at[1], trecv.at[1, k], {"y": part})

    def t_sib(k, kind, f):
        ref = xbuf.at[part_rows(k), block(f)]
        return remote(ref, ref, tsend.at[1], trecv.at[kind, k], sibling)

    def t_own():
        return remote(tok, xbuf.at[:, block(y)], tsend.at[0], trecv.at[2, 0], sibling)

    def t_wait(k, kind, f):
        t_sib(k, kind, f).wait_recv()

    def w_rows(xp, zp):
        return pl.ds(pl.multiple_of((xp * NZ + zp) * wr, wr), wr)

    far_block = rem(x + 2, NX)
    w_cols = (pl.ds(nh, 2 * hs), pl.ds(nh + 2 * hs, hs), pl.ds(nh + hs, hs))

    def w_piece(i):
        return remote(
            weights[i].at[w_rows(x, z), head(c)], wbuf.at[w_rows(x, z), pl.ds(nh + i * hs, hs)],
            wys.at[0], wyr.at[i // 2], {"y": cross},
        )

    def w_z(kind, d):
        ref = wbuf.at[w_rows(x, z), w_cols[kind]]
        return remote(ref, ref, wzs.at[0], wqr.at[0] if kind else wzr.at[d], zz(d))

    def w_x(kind, i, d):
        ref = wbuf.at[w_rows(x, rem(z + NZ - d, NZ)), w_cols[kind]]
        return remote(ref, ref, wxs.at[kind], wxr.at[kind], xx(i))

    def w_xs(d):
        w_x(0, 1, d).start()
        w_x(0, 3, d).start()

        @pl.when(c == 0)
        def _():
            w_x(2, 2, d).start()

    def w_cross(i, ct):
        return remote(
            weights[i].at[block(far_block), head(ct)], wbuf.at[block(far_block), pl.ds(nh + i * hs, hs)],
            wcs.at[0], wcr.at[i // 2], {"y": cross, "c": ct},
        )

    def o_rows(xp, zp):
        return pl.ds(pl.multiple_of((xp * NZ + zp) * br, br), br)

    def o_y():
        return remote(
            wo.at[o_rows(x, z), group(NY - 1 - gp)], wof.at[2, o_rows(x, z), :], o0s.at[0], o0r.at[0], yy(2)
        )

    def o_z(d):
        ref = wof.at[2, o_rows(x, z), :]
        return remote(ref, ref, o1s.at[0], o1r.at[0], zz(d))

    def o_x(i):
        ref = wof.at[2, pl.ds(pl.multiple_of(x * NZ * br, NZ * br), NZ * br), :]
        return remote(ref, ref, o2s.at[0], o2r.at[0], xx(i))

    def o_pair():
        return remote(
            wo.at[:, group(gp)], wof.at[3 - 2 * rem(y, 2)], o3s.at[0], o3r.at[0], {"y": part}
        )

    def o_cross():
        return remote(
            wo.at[:, group(NY - 1 - g)], wof.at[1 + 2 * rem(y, 2)], o3s.at[0], o3r.at[1], {"y": cross}
        )

    def g_copy():
        return remote(ls, lb, gsend.at[0], grecv.at[0], {"y": cross})

    for i in range(2):
        w_piece(i).start()
    o_y().start()

    @pl.when(is_source)
    def _():
        for k in range(nk):
            t_pair(k).start()
        t_own().start()

    @pl.when(not_source)
    def _():
        for k in range(nk):
            t_cross(k).start()

    w_piece(2).start()
    g_copy().start()

    @pl.when(not_source)
    def _():
        for i, ct in ((0, 1), (1, 1), (0, 0), (2, 1), (2, 0)):
            w_cross(i, ct).start()

    macc[...] = jnp.zeros_like(macc)
    nacc[...] = jnp.zeros_like(nacc)

    @pl.when(is_source)
    def _():
        done(xbuf.at[:, block(y)], lsem.at[0])

    @pl.when(not_source)
    def _():
        t_own().wait_recv()

    done(wbuf.at[:, pl.ds(0, nh)], lsem.at[1])

    def own_dot(j, carry):
        acc[chunk(j), 0:nh] = jnp.dot(
            xbuf[chunk(j), block(y)], wbuf[block(y), 0:nh], preferred_element_type=F32
        )
        return carry

    lax.fori_loop(0, 2, own_dot, 0)
    done(wbuf.at[pl.ds(0, wr), pl.ds(0, 2 * hs)], wyr.at[0])
    for d in ZORDER:
        w_z(0, d).start()
    w_xs(0)
    lax.fori_loop(2, 4, own_dot, 0)

    forward_at = {0: (1, 7), 1: (2, 6), 2: (3, 5), 3: (4,), 4: ()}
    for k in range(nk):
        t_wait(k, 3, cross)

        @pl.when(is_main)
        def _(k=k):
            t_on(k).start()
            t_sib(k, 3, cross).start()

        for d in forward_at[k]:
            w_z(0, d).wait_recv()
            w_xs(d)
        rows = part_rows(k)
        acc[rows, 0:nh] += jnp.dot(xbuf[rows, block(cross)], wbuf[block(cross), 0:nh], preferred_element_type=F32)

    def finish(h, rows, kv):
        kv = kv.astype(BF16)
        key, val = kv[:, :hs], kv[:, hs:]
        k_s[h, rows, :] = key
        v_s[h, rows, :] = val
        fk = feature(key.astype(F32)).astype(BF16)
        macc[h] += lax.dot_general(fk, val, TN, preferred_element_type=F32)
        nacc[h] += jnp.sum(fk.astype(F32).reshape(-1, 8, hs), axis=0)

    def cross_rows(k):
        rows = part_rows(k)
        kv = acc[rows, ck]
        for i in range(1, NX):
            f = block(rem(x + i, NX))
            kv += jnp.dot(xbuf[rows, f], wbuf[f, ck], preferred_element_type=F32)
        finish(1, rows, kv)

    done(wbuf.at[pl.ds(0, wr), pl.ds(0, hs)], wyr.at[1])
    for d in ZORDER:
        w_z(1, d).start()
    w_x(1, 1, 0).start()
    w_x(1, 3, 0).start()

    done(wof.at[2, pl.ds(0, br), :], o0r.at[0])
    for d in ZORDER:
        o_z(d).start()

    def q_forward():
        done(wbuf.at[pl.ds(0, wr * (NZ - 1)), pl.ds(0, hs)], wqr.at[0])
        for d in ZORDER:
            w_x(1, 1, d).start()
            w_x(1, 3, d).start()

    last = NY - 1 - part
    for k in range(nk):
        if k == 2:

            @pl.when(c == 1)
            def _():
                done(wbuf.at[pl.ds(0, 2 * NZ * wr), pl.ds(0, 2 * hs)], wxr.at[0])
                done(wbuf.at[pl.ds(0, fs), pl.ds(0, 2 * hs)], wcr.at[0])
                cross_rows(0)
                cross_rows(1)

        if k == 3:

            @pl.when(c == 0)
            def _():
                done(wbuf.at[pl.ds(0, 2 * NZ * wr), pl.ds(0, 2 * hs)], wxr.at[0])
                done(wbuf.at[pl.ds(0, fs), pl.ds(0, hs)], wxr.at[2])
                done(wbuf.at[pl.ds(0, fs), pl.ds(0, hs)], wcr.at[0])
                cross_rows(0)
                cross_rows(1)

            cross_rows(2)
            pl.when(c == 1)(q_forward)

        t_wait(k, 0, part)

        @pl.when(is_main)
        def _(k=k):
            t_sib(k, 0, part).start()

        t_wait(k, 1, last)

        @pl.when(is_main)
        def _(k=k):
            t_sib(k, 1, last).start()

        rows = part_rows(k)
        acc[rows, ck] = jnp.dot(xbuf[rows, block(x)], wbuf[block(x), ck], preferred_element_type=F32)
        add = jnp.dot(xbuf[rows, block(part)], wbuf[block(part), 0:nh], preferred_element_type=F32)
        kv = jnp.dot(xbuf[rows, block(last)], wbuf[block(last), ok], preferred_element_type=F32)
        acc[rows, oq] += add[:, oq]
        finish(0, rows, acc[rows, ok] + (kv + add[:, ok]))
        if k >= 3:
            cross_rows(k)

    per_head, hw = hs // pr, hs // 2
    norms = []
    for h in range(heads):
        slot = m if h == 0 else 1 - m
        norm = jnp.sum(nacc[h], axis=0, keepdims=True)
        which = lax.broadcasted_iota(jnp.int32, (16, hw), 0)
        norms += [jnp.where(which == 2 * slot + i, norm[:, i * hw : (i + 1) * hw], 0.0) for i in range(2)]
        for p in range(per_head):
            rows = slice(p * pr, (p + 1) * pr)
            for i in range(2):
                mt[slot * per_head + p, i * pr : (i + 1) * pr, :] = macc[h, rows, i * hw : (i + 1) * hw].astype(BF16)
    for p in range(NE):
        mt[p, 2 * pr :, :] = sum(norms).astype(BF16)

    def a_copy(i):
        return remote(mt.at[rem(e + i, NE)], ga.at[e], asend.at[0], arecv.at[0], ee(i))

    def b_copy(d):
        return remote(tb, gb.at[z], bsend.at[0], brecv.at[0], zz(d))

    def c_copy(i):
        return remote(pc.at[rem(e + i, NE)], gc.at[e], csend.at[0], crecv.at[0], ee(i))

    for i in range(1, NE):
        a_copy(i).start()
    ga[e] = mt[e]
    o_pair().start()

    @pl.when(not_source)
    def _():
        o_cross().start()

    pl.when(c == 0)(q_forward)

    scale = 1.0 / hs**0.5
    lower = lax.broadcasted_iota(jnp.int32, (rc, rc), 1) <= lax.broadcasted_iota(jnp.int32, (rc, rc), 0)

    def attend(h):
        for i in range(4):
            rows = slice(i * rc, (i + 1) * rc)
            q = q_s[h, rows, :]
            diag = lax.dot_general(q, k_s[h, rows, :], NT, preferred_element_type=F32) * scale
            diag = jnp.where(lower, diag, -1e30)
            top = jnp.max(diag, axis=1, keepdims=True)
            if i:
                before = lax.dot_general(q, k_s[h, 0 : i * rc, :], NT, preferred_element_type=F32) * scale
                top = jnp.maximum(top, jnp.max(before, axis=1, keepdims=True))
                pb = jnp.exp(before - top)
            pd = jnp.exp(diag - top)
            total = jnp.sum(pd, axis=1, keepdims=True)
            got = jnp.dot(pd.astype(BF16), v_s[h, rows, :], preferred_element_type=F32)
            if i:
                total += jnp.sum(pb, axis=1, keepdims=True)
                got += jnp.dot(pb.astype(BF16), v_s[h, 0 : i * rc, :], preferred_element_type=F32)
            loc[h, rows, :] = got / total * (1.0 - shares[h])

    def own_q(j, carry):
        rows = chunk(j)
        add = jnp.dot(xbuf[rows, block(last)], wbuf[block(last), oq], preferred_element_type=F32)
        q_s[0, rows, :] = (acc[rows, oq] + add).astype(BF16)
        return carry

    lax.fori_loop(0, 4, own_q, 0)
    shares = [jax.nn.sigmoid(ls[0:1, :])]
    attend(0)

    done(ga.at[pl.ds(0, NE - 1)], arecv.at[0])
    plane = ga[0].astype(F32)
    for p in range(1, NE):
        plane += ga[p].astype(F32)
    tb[...] = plane.astype(BF16)
    for d in (4, 3, 5, 2, 6, 1, 7):

        @pl.when(z + d < NZ)
        def _(d=d):
            b_copy(d).start()

    def bulk():
        @pl.when(is_source)
        def _():
            o_cross().start()

        for i in range(1, NX):
            o_x(i).start()

    done(wof.at[2, pl.ds(0, (NZ - 1) * br), :], o1r.at[0])

    done(wbuf.at[pl.ds(0, fs), pl.ds(0, hs)], wcr.at[1])
    done(wbuf.at[pl.ds(0, 2 * NZ * wr), pl.ds(0, hs)], wxr.at[1])
    g_copy().wait_recv()

    def cross_q(j, carry):
        rows = chunk(j)
        q_s[1, rows, :] = jnp.dot(xbuf[rows, :], wbuf[:, cq], preferred_element_type=F32).astype(BF16)
        return carry

    lax.fori_loop(0, 4, cross_q, 0)
    shares.append(jax.nn.sigmoid(lb[0:1, :]))

    attend(1)

    for n in range(1, NZ):

        @pl.when(z == n)
        def _(n=n):
            done(gb.at[pl.ds(0, n)], brecv.at[0])

    run = lax.fori_loop(0, z, lambda k, s: s + gb[k].astype(F32), jnp.zeros(tb.shape, F32))
    for p in range(NE):
        pc[p] = run.astype(BF16)
        run += ga[p].astype(F32)
    for i in range(1, NE):
        c_copy(i).start()
    gc[e] = pc[e]

    done(gc.at[pl.ds(0, NE - 1)], crecv.at[0])
    bulk()
    for h in range(heads):
        slot = m if h == 0 else 1 - m
        for p in range(per_head):
            for i in range(2):
                mem[h, p * pr : (p + 1) * pr, i * hw : (i + 1) * hw] = gc[slot * per_head + p, i * pr : (i + 1) * pr, :]
        for i in range(2):
            row = 2 * pr + i
            norm = jnp.where(slot == 0, gc[0, row : row + 1, :].astype(F32), gc[0, row + 2 : row + 3, :].astype(F32))
            nrm[h, :, i * hw : (i + 1) * hw] = jnp.broadcast_to(norm, (hs, hw)).astype(BF16)

    sizes = [seg // 8] * 7 + [seg // 16] * 2
    spans = [(sum(sizes[:u]), size) for u, size in enumerate(sizes)]

    pidx = div(y * cross, 2)

    def m_ref(u, cc, pp):
        return mixs.at[pl.ds(*spans[u]), pl.ds(pl.multiple_of(cc * 4 * hs + pp * 2 * hs, hs), 2 * hs)]

    def m_pair(u, pp):
        return remote(m_ref(u, c, pp), m_ref(u, c, pp), psend.at[0], precv.at[u], {"y": part})

    def m_sib(u, pp, fin):
        return remote(m_ref(u, c, pp), m_ref(u, c, pp), fin.at[0], drecv.at[u], sibling)

    for u in range(NU):
        rows = pl.ds(*spans[u])
        for h in range(heads):
            fq = feature(q_s[h, rows, :].astype(F32)).astype(BF16)
            denom = lax.dot_general(fq, nrm[h], NT, preferred_element_type=F32)
            numer = jnp.dot(fq, mem[h], preferred_element_type=F32)
            val = shares[h] * (numer / jnp.maximum(denom, 1.0)) + loc[h, rows, :]
            at = c * 4 * hs + pidx * 2 * hs + (m if h == 0 else 1 - m) * hs
            mixs[rows, pl.ds(pl.multiple_of(at, hs), hs)] = val.astype(BF16)
        m_pair(u, pidx).start()
        m_sib(u, pidx, dsend).start()

    def o_copy(u):
        rows = pl.ds(*spans[u])
        dev = {"y": y + c * (cross - y), "c": m}
        return remote(outs.at[rows, :], out.at[rows, :], osend.at[0], orecv.at[0], dev)

    for step in range(NU + 1):
        if step < NU:
            m_pair(step, 1 - pidx).wait_recv()
            m_sib(step, 1 - pidx, fsend).start()
        if step:
            u = step - 1
            if u == 0:
                done(wof.at[2, pl.ds(0, (NX - 1) * NZ * br), :], o2r.at[0])
                done(wof.at[0], o3r.at[0])
                done(wof.at[0], o3r.at[1])
                done(wof.at[0], lsem.at[2])
            rows = pl.ds(*spans[u])
            done(mixs.at[rows, pl.ds(0, 2 * gw)], drecv.at[u])
            o = jnp.zeros((spans[u][1], fs), F32)
            for cc in range(NC):
                for pos, grp in enumerate((0, 3, 1, 2)):
                    at = cc * 4 * hs + pos * hs
                    part_w = wof[rem(grp + NY - y, NY), cc * hs : (cc + 1) * hs, :]
                    o += jnp.dot(mixs[rows, at : at + hs], part_w, preferred_element_type=F32)
            outs[rows, :] = o.astype(BF16)

            @pl.when(at_home)
            def _(rows=rows):
                fetch(outs.at[rows, :], out.at[rows, :], 3)

            @pl.when(jnp.logical_not(at_home))
            def _(u=u):
                o_copy(u).start()

    @pl.when(at_home)
    def _():
        done(outs, lsem.at[3])

    @pl.when(jnp.logical_not(at_home))
    def _():
        done(outs, osend.at[0])

    @pl.when(jnp.logical_not(at_home))
    def _():
        done(outs, orecv.at[0])

    done(outs, psend.at[0])
    done(outs, dsend.at[0])
    done(outs, fsend.at[0])

    @pl.when(is_source)
    def _():
        done(xbuf.at[:, pl.ds(0, 2 * fs)], tsend.at[0])

    @pl.when(is_main)
    def _():
        done(xbuf, tsend.at[1])

    @pl.when(not_source)
    def _():
        done(xbuf.at[:, pl.ds(0, fs)], tsend.at[0])
        done(wbuf.at[pl.ds(0, fs), pl.ds(0, 5 * hs)], wcs.at[0])

    done(wbuf.at[pl.ds(0, wr), pl.ds(0, nh)], wys.at[0])
    done(wbuf.at[pl.ds(0, (NZ - 1) * wr), pl.ds(0, nh)], wzs.at[0])
    done(wbuf.at[pl.ds(0, 2 * NZ * wr), pl.ds(0, 2 * hs)], wxs.at[0])
    done(wbuf.at[pl.ds(0, 2 * NZ * wr), pl.ds(0, hs)], wxs.at[1])

    @pl.when(c == 0)
    def _():
        done(wbuf.at[pl.ds(0, fs), pl.ds(0, hs)], wxs.at[2])

    g_copy().wait_send()

    done(wof.at[2, pl.ds(0, br), :], o0s.at[0])
    done(wof.at[2, pl.ds(0, (NZ - 1) * br), :], o1s.at[0])
    done(wof.at[2, pl.ds(0, (NX - 1) * NZ * br), :], o2s.at[0])
    done(wof.at[pl.ds(0, 2)], o3s.at[0])
    done(ga.at[pl.ds(0, NE - 1)], asend.at[0])
    done(gc.at[pl.ds(0, NE - 1)], csend.at[0])
    for n in range(1, NZ):

        @pl.when(z == NZ - 1 - n)
        def _(n=n):
            done(gb.at[pl.ds(0, n)], bsend.at[0])


def on_device(tokens, w_query, w_key, w_value, w_out, mix_logit):
    seg, fs = tokens.shape
    heads = mix_logit.shape[0]
    gw = w_query.shape[1]
    hs = gw // heads
    pr = heads * hs // NE
    hbm = pl.BlockSpec(memory_space=pl.ANY)
    dma = pltpu.SemaphoreType.DMA
    return pl.pallas_call(
        kernel,
        out_shape=jax.ShapeDtypeStruct((seg, fs), BF16),
        in_specs=[hbm] * 5 + [pl.BlockSpec(memory_space=pltpu.SMEM)],
        out_specs=hbm,
        scratch_shapes=[
            pltpu.VMEM((seg, NY * fs), BF16),
            pltpu.VMEM((NY * fs, 3 * gw), BF16),
            pltpu.VMEM((seg, 3 * gw), F32),
            pltpu.VMEM((heads, seg, hs), BF16),
            pltpu.VMEM((heads, seg, hs), BF16),
            pltpu.VMEM((heads, seg, hs), BF16),
            pltpu.VMEM((heads, seg, hs), F32),
            pltpu.VMEM((NY, gw, fs), BF16),
            pltpu.VMEM((heads, hs, hs), F32),
            pltpu.VMEM((heads, 8, hs), F32),
            pltpu.VMEM((NE, 2 * pr + 16, hs // 2), BF16),
            pltpu.VMEM((NE, 2 * pr + 16, hs // 2), BF16),
            pltpu.VMEM((2 * pr + 16, hs // 2), BF16),
            pltpu.VMEM((NZ, 2 * pr + 16, hs // 2), BF16),
            pltpu.VMEM((NE, 2 * pr + 16, hs // 2), BF16),
            pltpu.VMEM((NE, 2 * pr + 16, hs // 2), BF16),
            pltpu.VMEM((heads, hs, hs), BF16),
            pltpu.VMEM((heads, hs, hs), BF16),
            pltpu.VMEM((seg, NY * gw), BF16),
            pltpu.VMEM((seg, fs), BF16),
            pltpu.VMEM((8, hs), F32),
            pltpu.VMEM((8, hs), F32),
            dma((4,)),
            dma((2,)), dma((4, 5)),
            dma((1,)), dma((2,)),
            dma((1,)), dma((NZ,)), dma((1,)),
            dma((3,)), dma((3,)),
            dma((1,)), dma((2,)),
            dma((1,)), dma((1,)),
            dma((1,)), dma((1,)),
            dma((1,)), dma((1,)),
            dma((1,)), dma((2,)),
            dma((1,)), dma((1,)),
            dma((1,)), dma((1,)),
            dma((1,)), dma((1,)),
            dma((1,)), dma((1,)),
            dma((1,)), dma((NU,)),
            dma((1,)), dma((NU,)),
            dma((1,)),
            dma((1,)), dma((1,)),
        ],
        compiler_params=pltpu.CompilerParams(
            collective_id=0, has_side_effects=True, vmem_limit_bytes=52 * 2**20
        ),
    )(tokens, w_query, w_key, w_value, w_out, mix_logit)


def solution(mesh):
    torus = Mesh(mesh.devices.reshape(NZ, NX, NC, NY), ("z", "x", "c", "y"))
    return jax.shard_map(
        on_device,
        mesh=torus,
        in_specs=(P(SEQ, "y"), P(None, "y"), P(None, "y"), P(None, "y"), P("y", None), P("y")),
        out_specs=P(SEQ, "y"),
        check_vma=False,
    )
```
